256 devices in a mesh: dp: 128 (over z, x, y), rep: 2 (over core).
Axes of the slice: x: 4, y: 4, z: 8, core: 2. Of those that a mesh axis runs over, the one named last changes fastest.
Arguments:
- ids: int32 [65536], P(('dp', 'rep')), may hold values from 0 to 65520
- counts: int32 [256], P(('dp', 'rep')), may hold values from 1 to 256, as said below
- hash_scale: int32 [512], replicated, may hold values from 1 to 32767
- hash_shift: int32 [512], replicated, may hold values from 0 to 65520
- w_code: bfloat16 [512, 1024], replicated, may hold values from -0.25 to 0.25
- norm_gain: float32 [1024], replicated, may hold values from 0.5 to 1.5
- norm_bias: float32 [1024], replicated, may hold values from -3 to 3
- w_out: bfloat16 [1024, 128], replicated, may hold values from -0.1875 to 0.1875
- out_bias: float32 [128], replicated, may hold values from -3 to 3
- cotangent: bfloat16 [65536, 128], P(('dp', 'rep')), may hold values from -6 to 6
Outputs:
- embeddings: bfloat16 [65536, 128], P(('dp', 'rep'))
- grad_code_t: float32 [1024, 512], P(('dp', 'rep'))
- grad_out: float32 [1024, 128], P(('dp', 'rep'))
- grad_gain: float32 [1024], replicated
- grad_bias: float32 [1024], replicated
The draws below stay inside these ranges and needn't reach their ends.
Inputs may be any that keep to these rules, and one draw needn't show every extreme that they name: Each device has 1 to 256 live slots, the first ones of its slots; the counts of the devices of one rep index sum to exactly 8192, and in each such group one device has exactly 256.
All inputs are finite; a program needn't handle non-finite values.
Results may differ from the reference program's by a relative error of at most 0.006.
Values may be sent and summed in bfloat16 or wider, within the bound.
A program may use at most 64 MiB of HBM per device.

```python
import math
import jax
import jax.numpy as jnp
import numpy as np
from jax import lax

CODES = 512
HID = 1024
OUT = 128
SLOTS = 256
SLOTS_ALL = 65536
LIVE_GROUP = 8192
LIVE_ALL = 16384
N_DP = 128
N_REP = 2


def draw_counts(key, part):
    groups = []
    for member in range(N_REP):
        group_key = jax.random.fold_in(key, 7919 + member)
        key_base, key_peak, key_order = jax.random.split(group_key, 3)
        device_index = jnp.arange(N_DP, dtype=jnp.int32)
        base_weight = jax.random.randint(key_base, (N_DP,), 1, 3).astype(jnp.int32)
        ramp_weight = N_DP - 1 + 2 * device_index
        peak_index = jax.random.randint(key_peak, (), 0, N_DP).astype(jnp.int32)
        weight = jnp.where(device_index == peak_index, 0, base_weight * ramp_weight)
        surplus = LIVE_GROUP - SLOTS - (N_DP - 1)
        portion = surplus * weight // jnp.sum(weight)
        counts = jnp.where(device_index == peak_index, SLOTS, 1 + portion).astype(jnp.int32)
        remainder = LIVE_GROUP - jnp.sum(counts)
        priority = jnp.where(device_index == peak_index, N_DP, jax.random.permutation(key_order, N_DP).astype(jnp.int32))
        position = jnp.argsort(jnp.argsort(priority))
        counts = counts + (position < remainder).astype(jnp.int32)
        groups.append(counts)
    return jnp.stack(groups, axis=1).reshape(-1).astype(jnp.int32)


def touch_ends(values, rng, low, top_value):
    spot = [jax.random.randint(jax.random.fold_in(rng, axis), (), 0, length) for axis, length in enumerate(values.shape)]
    main_axis = values.shape.index(max(values.shape))
    beside = spot[:main_axis] + [(spot[main_axis] + 1) % values.shape[main_axis]] + spot[main_axis + 1:]
    return values.at[tuple(spot)].set(low).at[tuple(beside)].set(top_value)


def level_of(stream_key, extent, cuts, smallest, top_value):
    def one(dim, parts):
        draws = jax.random.uniform(jax.random.fold_in(jax.random.fold_in(stream_key, 6), dim), (parts,), jnp.float32, smallest / len(cuts), top_value / len(cuts))
        return jnp.repeat(jnp.exp(draws), extent[dim] // parts).reshape((-1,) + (1,) * (len(extent) - dim - 1))

    level = one(*cuts[0])
    for cut in cuts[1:]:
        level = level * one(*cut)
    return level


def rank_table(count, lean):
    loads = [(1 << 20) // math.isqrt(grade ** lean) + 1 for grade in range(1, count + 1)]
    scale = 1 + sum(loads) // (1 << 30)
    return np.cumsum(np.array([max(1, weight // scale) for weight in loads]))


def skewed_ids(key, shape, count, lean):
    grid = rank_table(count, lean)
    lot = jax.random.randint(jax.random.fold_in(key, 1), shape, 0, int(grid[count - 1]))
    grade = jnp.searchsorted(jnp.asarray(grid, jnp.int32), lot, side="right")
    return jax.random.permutation(jax.random.fold_in(key, 2), count)[grade].astype(jnp.int32)


def centred(rng, extent, scale, limit, shards=(), kind=jnp.bfloat16):
    values = jax.random.normal(rng, extent, jnp.float32) * scale
    if len(shards) > 0:
        values = level_of(rng, extent, shards, -0.22, 0.18) * values
    return jnp.clip(values, min=-limit, max=limit).astype(kind)


def setup_inputs(seed: int = 0) -> dict:
    key_list = jax.random.split(jax.random.key(seed), 11)
    return {
        "ids": touch_ends(skewed_ids(key_list[0], (SLOTS_ALL,), 65521, 2), jax.random.fold_in(key_list[0], 3), 0, 65520).astype(jnp.int32),
        "counts": draw_counts(jax.random.fold_in(key_list[10], 71), 0),
        "hash_scale": touch_ends(jax.random.randint(key_list[2], (CODES,), 1, 32768), jax.random.fold_in(key_list[2], 1), 1, 32767).astype(jnp.int32),
        "hash_shift": touch_ends(jax.random.randint(key_list[3], (CODES,), 0, 65521), jax.random.fold_in(key_list[3], 1), 0, 65520).astype(jnp.int32),
        "w_code": centred(key_list[4], (CODES, HID), CODES ** -0.5, 0.25),
        "norm_gain": jnp.clip(jax.random.uniform(key_list[5], (HID,), jnp.float32, 0.5, 1.5), 0.5, 1.5),
        "norm_bias": centred(key_list[6], (HID,), 0.5, 3.0, (), jnp.float32),
        "w_out": centred(key_list[7], (HID, OUT), HID ** -0.5, 0.1875),
        "out_bias": centred(key_list[8], (OUT,), 0.5, 3.0, (), jnp.float32),
        "cotangent": centred(key_list[9], (SLOTS_ALL, OUT), 1.0, 6.0, ((0, 256),)),
    }


modulus = 65521
epsilon = 1e-05

def hashed(ident, hash_scale, hash_shift):
    resid = ident % modulus
    bucket = (hash_scale[None, :] * resid[:, None] + hash_shift[None, :]) % modulus
    return (bucket.astype(jnp.float32) * (2.0 / (modulus - 1)) - 1.0).astype(jnp.bfloat16)

def mish_parts(gated):
    softer = jax.nn.softplus(gated)
    tangent = jnp.tanh(softer)
    return (gated * tangent, tangent + gated * (1.0 - tangent * tangent) * jax.nn.sigmoid(gated))

def reference(ids, counts, hash_scale, hash_shift, w_code, norm_gain, norm_bias, w_out, out_bias, cotangent):
    width = w_out.shape[1]
    hidden = w_code.shape[1]
    owner_device = jnp.arange(SLOTS_ALL, dtype=jnp.int32) // SLOTS
    slot_index = jnp.arange(SLOTS_ALL, dtype=jnp.int32) % SLOTS
    is_live = slot_index < counts[owner_device]
    live_order = jnp.argsort(jnp.where(is_live, 0, 1).astype(jnp.int32), stable=True)[:LIVE_ALL]
    group_count = LIVE_ALL // 1024
    sel_ids = ids[live_order].reshape(group_count, 1024)
    sel_cot = cotangent[live_order].reshape(group_count, 1024, width)
    total = jnp.sum(counts).astype(jnp.float32)

    def forward(ident):
        code_rows = hashed(ident, hash_scale, hash_shift)
        return (code_rows, jnp.dot(code_rows, w_code, preferred_element_type=jnp.float32))

    def stats(state_carry, ident):
        preact = forward(ident)[1]
        return ((state_carry[0] + preact.sum(0), state_carry[1] + (preact * preact).sum(0)), None)
    zero_row = jnp.zeros((hidden,), jnp.float32)
    (sum_hidden, sum_square), _ = lax.scan(stats, (zero_row, zero_row), sel_ids)
    feature_mean = sum_hidden / total
    inv_std = lax.rsqrt(sum_square / total - feature_mean * feature_mean + epsilon)
    loss_scale = lax.rsqrt(total)

    def middle(ident, cot_rows):
        code_rows, preact = forward(ident)
        normed = (preact - feature_mean) * inv_std
        act_full, mish_slope = mish_parts(normed * norm_gain + norm_bias)
        activation = act_full.astype(jnp.bfloat16)
        delta_rows = (cot_rows.astype(jnp.float32) * loss_scale).astype(jnp.bfloat16)
        grad_act = lax.dot_general(delta_rows, w_out, (((1,), (1,)), ((), ())), preferred_element_type=jnp.float32)
        return (code_rows, normed, activation, delta_rows, grad_act * mish_slope)

    def second(state_carry, pair):
        code_rows, normed, activation, delta_rows, dvalue = middle(pair[0], pair[1])
        embedded = (jnp.dot(activation, w_out, preferred_element_type=jnp.float32) + out_bias).astype(jnp.bfloat16)
        out_part = lax.dot_general(activation, delta_rows, (((0,), (0,)), ((), ())), preferred_element_type=jnp.float32)
        return ((state_carry[0] + (dvalue * normed).sum(0), state_carry[1] + dvalue.sum(0), state_carry[2] + out_part), embedded)
    start_out = jnp.zeros((hidden, width), jnp.float32)
    (grad_gain, grad_bias, grad_out), embedded = lax.scan(second, (zero_row, zero_row, start_out), (sel_ids, sel_cot))

    def third(state_carry, pair):
        code_rows, normed, activation, delta_rows, dvalue = middle(pair[0], pair[1])
        dpre = (norm_gain * inv_std * (dvalue - grad_bias / total - normed * grad_gain / total)).astype(jnp.bfloat16)
        return (state_carry + lax.dot_general(dpre, code_rows, (((0,), (0,)), ((), ())), preferred_element_type=jnp.float32), None)
    grad_code_t, _ = lax.scan(third, jnp.zeros((hidden, w_code.shape[0]), jnp.float32), (sel_ids, sel_cot))
    embeddings = jnp.zeros((SLOTS_ALL, width), jnp.bfloat16).at[live_order].set(embedded.reshape(LIVE_ALL, width))
    return (embeddings, grad_code_t, grad_out, grad_gain, grad_bias)
```

```python
import functools

import jax
import jax.numpy as jnp
from jax import lax
from jax.experimental import pallas as pl
from jax.experimental.pallas import tpu as pltpu
from jax.sharding import Mesh
from jax.sharding import PartitionSpec as P

AXES = ("z", "x", "y", "c")
MESH = pl.DeviceIdType.MESH
F32 = jnp.float32
BF16 = jnp.bfloat16
MODULUS = 65521
EPSILON = 1e-05
TOTAL = 16384.0
ROWS = 256
CODES = 512
GROUP = 8
PEERS = 32

NN = (((1,), (0,)), ((), ()))
NT = (((1,), (1,)), ((), ()))
TN = (((0,), (0,)), ((), ()))


def dot(a, b, dims=NN):
    return lax.dot_general(a, b, dims, preferred_element_type=F32)


def exact_pick(values, onehot):
    high = values.astype(BF16)
    rest = values - high.astype(F32)
    mid = rest.astype(BF16)
    low = (rest - mid.astype(F32)).astype(BF16)
    return dot(high, onehot) + dot(mid, onehot) + dot(low, onehot)


def iota(shape, dim):
    return lax.broadcasted_iota(jnp.int32, shape, dim)


def hidden_pick(q):
    i = iota((128, 1024), 0)
    h = iota((128, 1024), 1)
    return jnp.where(h == (i // 4) * 32 + q * 4 + i % 4, 1.0, 0.0).astype(BF16)


def lane_pick(q):
    lane = iota((128, 128), 0)
    i = iota((128, 128), 1)
    return jnp.where(lane == ((i % 16) // 4) * 32 + q * 4 + i % 4, 1.0, 0.0).astype(BF16)


def lane_put(q):
    i = iota((128, 128), 0)
    lane = iota((128, 128), 1)
    return jnp.where(lane == ((i % 16) // 4) * 32 + q * 4 + i % 4, 1.0, 0.0).astype(BF16)


def mish_terms(val):
    u = jnp.exp(jnp.minimum(val, 20.0))
    n = u * (u + 2.0)
    r = 1.0 / (n + 2.0)
    return u, n, r


def kernel(
    ids_ref, count_ref, scale_ref, shift_ref, wcode_ref, gain_ref, bias_ref, wout_ref, obias_ref, cot_ref,
    emb_ref, gcode_ref, gout_ref, ggain_ref, gbias_ref,
    idf, delta, code, pre, gact, dval, act, wown, wout_own, vec,
    st, st2, par, tot, p_send, p_recv, a_send, a_recv,
    s_id, r_id, s_dl, r_dl, s_st, r_st, s_p, r_p, s_par, r_par, s_st2, r_st2, s_a, r_a, s_tot, r_tot,
):
    z, x, y, c = (lax.axis_index(a) for a in AXES)
    q = y * 2 + c
    zx = z * 4 + x

    def far(k):
        t = lax.rem(zx + k, PEERS)
        return (t // 4, lax.rem(t, 4), y, c), t

    def near(k):
        t = lax.rem(q + k, GROUP)
        return (z, x, t // 2, lax.rem(t, 2)), t

    barrier = pltpu.get_barrier_semaphore()

    def greet_far(k, _):
        pl.semaphore_signal(barrier, inc=1, device_id=far(k)[0], device_id_type=MESH)
        return 0

    def greet_near(k, _):
        pl.semaphore_signal(barrier, inc=1, device_id=near(k)[0], device_id_type=MESH)
        return 0

    lax.fori_loop(1, GROUP, greet_near, 0)
    lax.fori_loop(1, PEERS, greet_far, 0)

    def to_near(buf, send, recv):
        def go(k, _):
            pltpu.make_async_remote_copy(
                buf.at[q], buf.at[q], send, recv, device_id=near(k)[0], device_id_type=MESH
            ).start()
            return 0

        lax.fori_loop(1, GROUP, go, 0)

    def to_far(buf, send, recv):
        def go(k, _):
            pltpu.make_async_remote_copy(
                buf.at[zx], buf.at[zx], send, recv, device_id=far(k)[0], device_id_type=MESH
            ).start()
            return 0

        lax.fori_loop(1, PEERS, go, 0)

    def scatter_far(src, dst, send, recv):
        def go(k, _):
            where, t = far(k)
            pltpu.make_async_remote_copy(
                src.at[t // 2, lax.rem(t, 2)], dst.at[zx], send, recv, device_id=where, device_id_type=MESH
            ).start()
            return 0

        lax.fori_loop(1, PEERS, go, 0)

    def wait(buf, n, sem):
        part = buf.at[pl.ds(0, n)]
        pltpu.make_async_copy(part, part, sem).wait()

    count = count_ref[0]
    slot = iota((2, 128), 0) * 128 + iota((2, 128), 1)
    idf[q] = jnp.where(slot < count, ids_ref[...].astype(F32), -1.0)
    live = iota((ROWS, 128), 0) < count
    delta[q] = jnp.where(live, cot_ref[...].astype(F32) * (1.0 / 128.0), 0.0).astype(BF16)

    pick = hidden_pick(q)
    wown[...] = dot(wcode_ref[...], pick, NT).astype(BF16)
    wout_own[...] = dot(pick, wout_ref[...]).astype(BF16)
    small = lane_pick(q)
    own_z = iota((8, 128), 0) == iota((8, 128), 1) // 16
    vec[0:1] = jnp.sum(jnp.where(own_z, exact_pick(gain_ref[...], small), 0.0), axis=0, keepdims=True)
    vec[1:2] = jnp.sum(jnp.where(own_z, exact_pick(bias_ref[...], small), 0.0), axis=0, keepdims=True)

    pl.semaphore_wait(barrier, PEERS - 1 + GROUP - 1)
    to_near(idf, s_id, r_id)
    to_near(delta, s_dl, r_dl)

    eye = iota((128, 128), 0) == iota((128, 128), 1)

    def hash_rows(qq, carry):
        total, square = carry
        for half in range(2):
            row = idf[qq, half : half + 1, :]
            ident = jnp.sum(jnp.where(eye, row, 0.0), axis=1, keepdims=True)
            alive = ident >= 0.0
            resid = ident.astype(jnp.int32)
            mixed = scale_ref[...] * resid + shift_ref[...]
            folded = (mixed & 65535) + 15 * lax.shift_right_logical(mixed, 16)
            value = folded.astype(F32)
            times = jnp.floor((value + 0.5) * (1.0 / MODULUS))
            bucket = value - times * float(MODULUS)
            rows = jnp.where(alive, bucket * (2.0 / (MODULUS - 1)) - 1.0, 0.0).astype(BF16)
            at = pl.multiple_of(qq * ROWS + half * 128, 128)
            code[pl.ds(at, 128), :] = rows
            hidden = dot(rows, wown[...])
            pre[pl.ds(at, 128), :] = hidden
            total = total + jnp.sum(hidden, axis=0, keepdims=True)
            square = square + jnp.sum(hidden * hidden, axis=0, keepdims=True)
        return total, square

    zero = jnp.zeros((1, 128), F32)
    sums = hash_rows(q, (zero, zero))
    wait(idf, GROUP - 1, r_id)
    sums = lax.fori_loop(1, GROUP, lambda k, s: hash_rows(near(k)[1], s), sums)
    st[zx] = jnp.concatenate(sums, axis=0)
    to_far(st, s_st, r_st)

    def stacked(full, lo):
        tiles = full.reshape(16, 8, full.shape[1])
        part = tiles[:, lo : lo + 4, :]
        return jnp.concatenate([part[:, :, :256], part[:, :, 256:]], axis=1)

    p_full = dot(pre[...].astype(BF16), code[...], TN)
    for parity in range(2):
        p_send[:, parity] = stacked(p_full, parity * 4).astype(BF16)
    p_recv[zx] = p_send[zx // 2, lax.rem(zx, 2)]
    scatter_far(p_send, p_recv, s_p, r_p)
    code_sum = dot(jnp.ones((8, GROUP * ROWS), BF16), code[...])[0:1]

    wait(delta, GROUP - 1, r_dl)

    def back_rows(b, _):
        at = pl.multiple_of(b * ROWS, ROWS)
        gact[pl.ds(at, ROWS), :] = dot(delta[b], wout_own[...], NT)
        return 0

    lax.fori_loop(0, GROUP, back_rows, 0)

    wait(st, PEERS - 1, r_st)
    moments = jnp.sum(st[...], axis=0) * (1.0 / TOTAL)
    mean = moments[0:1]
    inv_std = lax.rsqrt(moments[1:2] - mean * mean + EPSILON)
    gain = vec[0:1]
    bias = vec[1:2]
    par[q] = jnp.concatenate([mean, inv_std * gain, bias, bias], axis=0)
    to_near(par, s_par, r_par)

    def second(b, carry):
        sum_gain, sum_bias = carry
        at = pl.multiple_of(b * ROWS, ROWS)
        normed = (pre[pl.ds(at, ROWS), :] - mean) * inv_std
        val = normed * gain + bias
        u, n, r = mish_terms(val)
        act[b] = (val * (n * r)).astype(BF16)
        slope = r * (n + 4.0 * val * (u * (1.0 + u)) * r)
        d = gact[pl.ds(at, ROWS), :] * slope
        dval[pl.ds(at, ROWS), :] = d.astype(BF16)
        return (
            sum_gain + jnp.sum(d * normed, axis=0, keepdims=True),
            sum_bias + jnp.sum(d, axis=0, keepdims=True),
        )

    sums = lax.fori_loop(0, GROUP, second, (zero, zero))
    st2[zx] = jnp.concatenate(sums, axis=0)
    to_far(st2, s_st2, r_st2)

    a_full = dot(dval[...], code[...], TN)
    o_full = dot(act[...].reshape(GROUP * ROWS, 128), delta[...].reshape(GROUP * ROWS, 128), TN)
    s_rows = jnp.concatenate([code_sum[:, 128 * i : 128 * i + 128] for i in range(4)], axis=0)
    s_tiles = jnp.broadcast_to(s_rows[None], (16, 4, 128))
    o_tiles = o_full.reshape(16, 8, 128)
    for parity in range(2):
        a_send[:, parity, :, 0:256] = stacked(a_full, parity * 4).astype(BF16)
        both = jnp.concatenate([o_tiles[:, parity * 4 : parity * 4 + 4, :], s_tiles], axis=1)
        a_send[:, parity, :, 256:384] = both.astype(BF16)
    a_recv[zx] = a_send[zx // 2, lax.rem(zx, 2)]
    scatter_far(a_send, a_recv, s_a, r_a)

    wait(par, GROUP - 1, r_par)
    own_at = pl.multiple_of(q * ROWS, ROWS)

    def embed(k, acc):
        unit = hidden_pick(k)
        weights = dot(wcode_ref[...], unit, NT).astype(BF16)
        outward = dot(unit, wout_ref[...]).astype(BF16)
        hidden = dot(code[pl.ds(own_at, ROWS), :], weights)
        p = par[k]
        val = (hidden - p[0:1]) * p[1:2] + p[2:3]
        _, n, r = mish_terms(val)
        return acc + dot((val * (n * r)).astype(BF16), outward)

    acc = lax.fori_loop(0, GROUP, embed, jnp.zeros((ROWS, 128), F32))
    live = iota((ROWS, 128), 0) < count
    emb_ref[...] = jnp.where(live, acc + obias_ref[...], 0.0).astype(BF16)

    wait(st2, PEERS - 1, r_st2)
    sums = jnp.sum(st2[...], axis=0)
    tot[q] = sums
    to_near(tot, s_tot, r_tot)

    k1 = inv_std * gain
    k3 = k1 * inv_std * sums[0:1] * (1.0 / TOTAL)
    k2 = k1 * sums[1:2] * (1.0 / TOTAL) - k3 * mean
    mine = iota((8, 128), 1) == zx * 4 + iota((8, 128), 0) % 4

    def column(v):
        return jnp.sum(jnp.where(mine, v, 0.0), axis=1, keepdims=True)

    wait(p_recv, PEERS - 1, r_p)
    p_sum = jnp.sum(p_recv[...].astype(F32), axis=0)
    wait(a_recv, PEERS - 1, r_a)
    a_sum = jnp.sum(a_recv[...].astype(F32), axis=0)
    s_all = a_sum[4:8, 256:384]
    upper = jnp.concatenate([s_all[0:1], s_all[1:2]], axis=1)
    lower = jnp.concatenate([s_all[2:3], s_all[3:4]], axis=1)
    s_both = jnp.where(iota((8, 256), 0) < 4, upper, lower)
    grad = column(k1) * a_sum[:, 0:256] - column(k2) * s_both - column(k3) * p_sum
    gcode_ref[...] = jnp.concatenate([grad[0:4], grad[4:8]], axis=1)
    gout_ref[...] = a_sum[0:4, 256:384]

    wait(tot, GROUP - 1, r_tot)
    in_gain = jnp.zeros((8, 128), F32)
    in_bias = jnp.zeros((8, 128), F32)
    for k in range(GROUP):
        put = lane_put(k)
        t = tot[k]
        in_gain = in_gain + exact_pick(jnp.where(own_z, t[0:1], 0.0), put)
        in_bias = in_bias + exact_pick(jnp.where(own_z, t[1:2], 0.0), put)
    ggain_ref[...] = in_gain
    gbias_ref[...] = in_bias

    wait(idf, GROUP - 1, s_id)
    wait(delta, GROUP - 1, s_dl)
    wait(st, PEERS - 1, s_st)
    wait(p_recv, PEERS - 1, s_p)
    wait(par, GROUP - 1, s_par)
    wait(st2, PEERS - 1, s_st2)
    wait(a_recv, PEERS - 1, s_a)
    wait(tot, GROUP - 1, s_tot)


def per_device(ids, counts, hash_scale, hash_shift, w_code, norm_gain, norm_bias, w_out, out_bias, cotangent):
    vmem = pl.BlockSpec(memory_space=pltpu.VMEM)
    smem = pl.BlockSpec(memory_space=pltpu.SMEM)
    dma = pltpu.SemaphoreType.DMA
    wide = GROUP * ROWS
    emb, gcode, gout, ggain, gbias = pl.pallas_call(
        kernel,
        out_shape=(
            jax.ShapeDtypeStruct((ROWS, 128), BF16),
            jax.ShapeDtypeStruct((4, CODES), F32),
            jax.ShapeDtypeStruct((4, 128), F32),
            jax.ShapeDtypeStruct((8, 128), F32),
            jax.ShapeDtypeStruct((8, 128), F32),
        ),
        in_specs=[vmem, smem] + [vmem] * 8,
        out_specs=(vmem,) * 5,
        scratch_shapes=[
            pltpu.VMEM((GROUP, 2, 128), F32),
            pltpu.VMEM((GROUP, ROWS, 128), BF16),
            pltpu.VMEM((wide, CODES), BF16),
            pltpu.VMEM((wide, 128), F32),
            pltpu.VMEM((wide, 128), F32),
            pltpu.VMEM((wide, 128), BF16),
            pltpu.VMEM((GROUP, ROWS, 128), BF16),
            pltpu.VMEM((CODES, 128), BF16),
            pltpu.VMEM((128, 128), BF16),
            pltpu.VMEM((8, 128), F32),
            pltpu.VMEM((PEERS, 2, 128), F32),
            pltpu.VMEM((PEERS, 2, 128), F32),
            pltpu.VMEM((GROUP, 4, 128), F32),
            pltpu.VMEM((GROUP, 2, 128), F32),
            pltpu.VMEM((16, 2, 8, 256), BF16),
            pltpu.VMEM((PEERS, 8, 256), BF16),
            pltpu.VMEM((16, 2, 8, 384), BF16),
            pltpu.VMEM((PEERS, 8, 384), BF16),
        ]
        + [dma] * 16,
        compiler_params=pltpu.CompilerParams(
            collective_id=0, has_side_effects=True, vmem_limit_bytes=48 << 20
        ),
    )(
        ids.reshape(2, 128),
        counts,
        hash_scale.reshape(1, CODES),
        hash_shift.reshape(1, CODES),
        w_code,
        norm_gain.reshape(8, 128),
        norm_bias.reshape(8, 128),
        w_out,
        out_bias.reshape(1, 128),
        cotangent,
    )
    return emb, gcode, gout, ggain.reshape(1024), gbias.reshape(1024)


def solution(mesh):
    finer = Mesh(mesh.devices.reshape(8, 4, 4, 2), AXES)
    return jax.shard_map(
        per_device,
        mesh=finer,
        in_specs=(P(AXES), P(AXES), P(), P(), P(), P(), P(), P(), P(), P(AXES, None)),
        out_specs=(P(AXES, None), P(AXES, None), P(AXES, None), P(), P()),
        check_vma=False,
    )
```

```python
import functools

import jax
import jax.numpy as jnp
from jax import lax
from jax.experimental import pallas as pl
from jax.experimental.pallas import tpu as pltpu
from jax.sharding import Mesh
from jax.sharding import PartitionSpec as P

AXES = ("z", "x", "y", "c")
MESH = pl.DeviceIdType.MESH
F32 = jnp.float32
BF16 = jnp.bfloat16
MODULUS = 65521
EPSILON = 1e-05
MAGIC = 12582912.0
TOTAL = 16384.0
ROWS = 256
CODES = 512
GROUP = 8
PEERS = 32

NN = (((1,), (0,)), ((), ()))
NT = (((1,), (1,)), ((), ()))
TN = (((0,), (0,)), ((), ()))


def dot(a, b, dims=NN):
    return lax.dot_general(a, b, dims, preferred_element_type=F32)


def iota(shape, dim):
    return lax.broadcasted_iota(jnp.int32, shape, dim)


def parts(values):
    high = values.astype(BF16)
    rest = values - high.astype(F32)
    mid = rest.astype(BF16)
    low = (rest - mid.astype(F32)).astype(BF16)
    return high, mid, low


def exact_pick(values, onehot):
    high, mid, low = parts(values)
    return dot(high, onehot) + dot(mid, onehot) + dot(low, onehot)


def hidden_pick(q):
    i = iota((128, 1024), 0)
    h = iota((128, 1024), 1)
    return jnp.where(h == (i // 4) * 32 + q * 4 + i % 4, 1.0, 0.0).astype(BF16)


def lane_pick(q):
    lane = iota((128, 128), 0)
    i = iota((128, 128), 1)
    return jnp.where(lane == ((i % 16) // 4) * 32 + q * 4 + i % 4, 1.0, 0.0).astype(BF16)


def lane_put(q):
    i = iota((128, 128), 0)
    lane = iota((128, 128), 1)
    return jnp.where(lane == ((i % 16) // 4) * 32 + q * 4 + i % 4, 1.0, 0.0).astype(BF16)


def mish_terms(val):
    u = jnp.exp(jnp.minimum(val, 20.0))
    n = u * (u + 2.0)
    r = 1.0 / (n + 2.0)
    return u, n, r


def kernel(
    count_ref, ids_hbm, scale_hbm, shift_hbm, gain_hbm, bias_hbm, wcode_hbm, wout_hbm, cot_hbm, obias_hbm,
    emb_ref, gcode_ref, gout_ref, ggain_ref, gbias_ref,
    ids_ref, scale_ref, shift_ref, gain_ref, bias_ref, wcode_ref, wout_ref, cot_ref, obias_ref, s_in,
    idf, delta, code, pre, gact, dval, act, wown, wout_own, vec, put, mix, nat,
    st, st2, par, tot, p_send, p_recv, a_send, a_recv,
    s_id, r_id, s_dl, r_dl, s_st, r_st, s_p, r_p, s_par, r_par, s_st2, r_st2, s_a, r_a, s_tot, r_tot,
):
    z, x, y, c = (lax.axis_index(a) for a in AXES)
    q = y * 2 + c
    zx = z * 4 + x

    def fold(m):
        return (m // 2 + m % 2) * (1 - 2 * (m % 2))

    def far(k):
        tz = lax.rem(z + 4 + fold(k // 4) + 8, 8)
        tx = lax.rem(x + 2 + fold(k % 4) + 4, 4)
        return (tz, tx, y, c), tz * 4 + tx

    def near(k):
        m = k // 2
        ty = lax.rem(y + m + (m // 2) * (5 - 2 * m), 4)
        tc = lax.rem(c + k % 2, 2)
        return (z, x, ty, tc), ty * 2 + tc

    loads = [
        pltpu.make_async_copy(src, dst, s_in.at[i])
        for i, (src, dst) in enumerate(
            (
                (ids_hbm, ids_ref),
                (cot_hbm, cot_ref),
                (wcode_hbm, wcode_ref),
                (wout_hbm, wout_ref),
                (scale_hbm, scale_ref),
                (shift_hbm, shift_ref),
                (gain_hbm, gain_ref),
                (bias_hbm, bias_ref),
                (obias_hbm, obias_ref),
            )
        )
    ]
    for load in loads:
        load.start()

    barrier = pltpu.get_barrier_semaphore()

    def greet_far(k, _):
        pl.semaphore_signal(barrier, inc=1, device_id=far(k)[0], device_id_type=MESH)
        return 0

    def greet_near(k, _):
        pl.semaphore_signal(barrier, inc=1, device_id=near(k)[0], device_id_type=MESH)
        return 0

    lax.fori_loop(0, PEERS - 1, greet_far, 0)
    lax.fori_loop(1, GROUP, greet_near, 0)

    def to_near(buf, send, recv):
        def go(k, _):
            pltpu.make_async_remote_copy(
                buf.at[q], buf.at[q], send, recv, device_id=near(k)[0], device_id_type=MESH
            ).start()
            return 0

        lax.fori_loop(1, GROUP, go, 0)

    def to_far(buf, send, recv):
        def go(k, _):
            pltpu.make_async_remote_copy(
                buf.at[zx], buf.at[zx], send, recv, device_id=far(k)[0], device_id_type=MESH
            ).start()
            return 0

        lax.fori_loop(0, PEERS - 1, go, 0)

    def scatter_far(src, dst, send, recv):
        def go(k, _):
            where, t = far(k)
            pltpu.make_async_remote_copy(
                src.at[t // 2, lax.rem(t, 2)], dst.at[zx], send, recv, device_id=where, device_id_type=MESH
            ).start()
            return 0

        lax.fori_loop(0, PEERS - 1, go, 0)

    def wait(buf, n, sem):
        part = buf.at[pl.ds(0, n)]
        pltpu.make_async_copy(part, part, sem).wait()

    count = count_ref[0]
    loads[0].wait()
    slot = iota((2, 128), 0) * 128 + iota((2, 128), 1)
    idf[q] = jnp.where(slot < count, ids_ref[...].astype(F32), -1.0)
    pl.semaphore_wait(barrier, PEERS - 1 + GROUP - 1)
    to_near(idf, s_id, r_id.at[q])

    loads[1].wait()
    live = iota((ROWS, 128), 0) < count
    delta[q] = jnp.where(live, cot_ref[...].astype(F32) * (1.0 / 128.0), 0.0).astype(BF16)
    to_near(delta, s_dl, r_dl)

    for load in loads[2:]:
        load.wait()
    pick = hidden_pick(q)
    wown[...] = dot(wcode_ref[...], pick, NT).astype(BF16)

    scale = scale_ref[...].astype(F32)
    high = scale * 256.0
    mix[0:1] = high - ((high * (1.0 / MODULUS) + MAGIC) - MAGIC) * float(MODULUS)
    mix[1:2] = scale
    mix[2:3] = shift_ref[...].astype(F32)

    eye = iota((128, 128), 0) == iota((128, 128), 1)

    def hash_rows(qq, carry):
        total, square = carry
        pair = idf[qq]
        ident = jnp.concatenate(
            [jnp.sum(jnp.where(eye, pair[h : h + 1], 0.0), axis=1, keepdims=True) for h in range(2)], axis=0
        )
        upper = jnp.floor(ident * (1.0 / 256.0))
        lower = ident - upper * 256.0
        value = mix[0:1] * upper + (mix[1:2] * lower + mix[2:3])
        times = (value * (1.0 / MODULUS) + MAGIC) - MAGIC
        bucket = value - times * float(MODULUS)
        bucket = jnp.where(bucket < 0.0, bucket + float(MODULUS), bucket)
        rows = (bucket * (2.0 / (MODULUS - 1)) - 1.0).astype(BF16)
        at = pl.multiple_of(qq * ROWS, ROWS)
        code[pl.ds(at, ROWS), :] = rows
        hidden = jnp.where(ident >= 0.0, dot(rows, wown[...]), 0.0)
        pre[pl.ds(at, ROWS), :] = hidden
        total = total + jnp.sum(hidden, axis=0, keepdims=True)
        square = square + jnp.sum(hidden * hidden, axis=0, keepdims=True)
        return total, square

    def hash_next(k, sums):
        other = near(k)[1]
        pltpu.make_async_copy(idf.at[other], idf.at[other], r_id.at[other]).wait()
        return hash_rows(other, sums)

    zero = jnp.zeros((1, 128), F32)
    sums = hash_rows(q, (zero, zero))
    wout_own[...] = dot(pick, wout_ref[...]).astype(BF16)
    small = lane_pick(q)
    own_z = iota((8, 128), 0) == iota((8, 128), 1) // 16
    vec[0:1] = jnp.sum(jnp.where(own_z, exact_pick(gain_ref[...], small), 0.0), axis=0, keepdims=True)
    vec[1:2] = jnp.sum(jnp.where(own_z, exact_pick(bias_ref[...], small), 0.0), axis=0, keepdims=True)
    sums = lax.fori_loop(1, GROUP, hash_next, sums)
    st[zx] = jnp.concatenate(sums, axis=0)
    to_far(st, s_st, r_st)

    def stacked(full, lo):
        tiles = full.reshape(16, 8, full.shape[1])
        part = tiles[:, lo : lo + 4, :]
        return jnp.concatenate([part[:, :, :256], part[:, :, 256:]], axis=1)

    p_full = dot(pre[...].astype(BF16), code[...], TN)
    for parity in range(2):
        p_send[:, parity] = stacked(p_full, parity * 4).astype(BF16)
    p_recv[zx] = p_send[zx // 2, lax.rem(zx, 2)]
    scatter_far(p_send, p_recv, s_p, r_p)
    alive = jnp.concatenate([jnp.where(idf[b, h : h + 1, :] >= 0.0, 1.0, 0.0) for b in range(8) for h in range(2)], axis=1)
    code_sum = dot(jnp.broadcast_to(alive, (8, GROUP * ROWS)).astype(BF16), code[...])[0:1]
    for b in range(GROUP):
        put[b * 128 : b * 128 + 128, :] = lane_put(b)

    wait(delta, GROUP - 1, r_dl)

    def back_rows(b, _):
        at = pl.multiple_of(b * ROWS, ROWS)
        gact[pl.ds(at, ROWS), :] = dot(delta[b], wout_own[...], NT)
        return 0

    lax.fori_loop(0, GROUP, back_rows, 0)

    def in_order(ref):
        blocks = [
            jnp.concatenate([jnp.where(own_z, ref[b, v : v + 1, :], 0.0) for b in range(GROUP)], axis=1) for v in range(2)
        ]
        out = dot(jnp.concatenate(parts(jnp.concatenate(blocks, axis=0)), axis=0), put[...])
        return out[0:16] + out[16:32] + out[32:48]

    wait(st, PEERS - 1, r_st)
    moments = jnp.sum(st[...], axis=0) * (1.0 / TOTAL)
    mean = moments[0:1]
    inv_std = lax.rsqrt(moments[1:2] - mean * mean + EPSILON)
    gain = vec[0:1]
    bias = vec[1:2]
    par[q] = jnp.concatenate([mean, inv_std], axis=0)
    to_near(par, s_par, r_par)

    def second(b, carry):
        sum_gain, sum_bias = carry
        at = pl.multiple_of(b * ROWS, ROWS)
        normed = (pre[pl.ds(at, ROWS), :] - mean) * inv_std
        val = normed * gain + bias
        u, n, r = mish_terms(val)
        act[b] = (val * (n * r)).astype(BF16)
        slope = r * (n + 4.0 * val * (u * (1.0 + u)) * r)
        d = gact[pl.ds(at, ROWS), :] * slope
        dval[pl.ds(at, ROWS), :] = d.astype(BF16)
        return (
            sum_gain + jnp.sum(d * normed, axis=0, keepdims=True),
            sum_bias + jnp.sum(d, axis=0, keepdims=True),
        )

    sums = lax.fori_loop(0, GROUP, second, (zero, zero))
    st2[zx] = jnp.concatenate(sums, axis=0)
    to_far(st2, s_st2, r_st2)

    a_full = dot(dval[...], code[...], TN)
    o_full = dot(act[...].reshape(GROUP * ROWS, 128), delta[...].reshape(GROUP * ROWS, 128), TN)
    s_rows = jnp.concatenate([code_sum[:, 128 * i : 128 * i + 128] for i in range(4)], axis=0)
    s_tiles = jnp.broadcast_to(s_rows[None], (16, 4, 128))
    o_tiles = o_full.reshape(16, 8, 128)
    for parity in range(2):
        a_send[:, parity, :, 0:256] = stacked(a_full, parity * 4).astype(BF16)
        both = jnp.concatenate([o_tiles[:, parity * 4 : parity * 4 + 4, :], s_tiles], axis=1)
        a_send[:, parity, :, 256:384] = both.astype(BF16)
    a_recv[zx] = a_send[zx // 2, lax.rem(zx, 2)]
    scatter_far(a_send, a_recv, s_a, r_a)

    wait(par, GROUP - 1, r_par)
    ordered = in_order(par)
    nat[0] = ordered[0:8]
    nat[1] = ordered[8:16] * gain_ref[...]
    own_at = pl.multiple_of(q * ROWS, ROWS)

    def embed(k, acc):
        at = pl.multiple_of(k * 128, 128)
        hidden = dot(code[pl.ds(own_at, ROWS), :], wcode_ref[:, pl.ds(at, 128)])
        val = (hidden - nat[0, pl.ds(k, 1), :]) * nat[1, pl.ds(k, 1), :] + bias_ref[pl.ds(k, 1), :]
        _, n, r = mish_terms(val)
        return acc + dot((val * (n * r)).astype(BF16), wout_ref[pl.ds(at, 128), :])

    acc = lax.fori_loop(0, GROUP, embed, jnp.zeros((ROWS, 128), F32))
    live = iota((ROWS, 128), 0) < count
    emb_ref[...] = jnp.where(live, acc + obias_ref[...], 0.0).astype(BF16)

    wait(st2, PEERS - 1, r_st2)
    sums = jnp.sum(st2[...], axis=0)
    tot[q] = sums
    to_near(tot, s_tot, r_tot)

    k1 = inv_std * gain
    k3 = k1 * inv_std * sums[0:1] * (1.0 / TOTAL)
    k2 = k1 * sums[1:2] * (1.0 / TOTAL) - k3 * mean
    mine = iota((8, 128), 1) == zx * 4 + iota((8, 128), 0) % 4

    def column(v):
        return jnp.sum(jnp.where(mine, v, 0.0), axis=1, keepdims=True)

    wait(p_recv, PEERS - 1, r_p)
    p_sum = jnp.sum(p_recv[...].astype(F32), axis=0)
    wait(a_recv, PEERS - 1, r_a)
    a_sum = jnp.sum(a_recv[...].astype(F32), axis=0)
    s_all = a_sum[4:8, 256:384]
    upper = jnp.concatenate([s_all[0:1], s_all[1:2]], axis=1)
    lower = jnp.concatenate([s_all[2:3], s_all[3:4]], axis=1)
    s_both = jnp.where(iota((8, 256), 0) < 4, upper, lower)
    grad = column(k1) * a_sum[:, 0:256] - column(k2) * s_both - column(k3) * p_sum
    gcode_ref[...] = jnp.concatenate([grad[0:4], grad[4:8]], axis=1)
    gout_ref[...] = a_sum[0:4, 256:384]

    wait(tot, GROUP - 1, r_tot)
    ordered = in_order(tot)
    ggain_ref[...] = ordered[0:8]
    gbias_ref[...] = ordered[8:16]

    wait(idf, GROUP - 1, s_id)
    wait(delta, GROUP - 1, s_dl)
    wait(st, PEERS - 1, s_st)
    wait(p_recv, PEERS - 1, s_p)
    wait(par, GROUP - 1, s_par)
    wait(st2, PEERS - 1, s_st2)
    wait(a_recv, PEERS - 1, s_a)
    wait(tot, GROUP - 1, s_tot)


def store_kernel(*refs):
    srcs, dsts, sem = refs[:5], refs[5:10], refs[10]
    copies = [pltpu.make_async_copy(a, b, sem.at[i]) for i, (a, b) in enumerate(zip(srcs, dsts))]
    for copy in copies:
        copy.start()
    for copy in copies:
        copy.wait()


def per_device(ids, counts, hash_scale, hash_shift, w_code, norm_gain, norm_bias, w_out, out_bias, cotangent):
    vmem = pl.BlockSpec(memory_space=pltpu.VMEM)
    hbm = pl.BlockSpec(memory_space=pltpu.HBM)
    dma = pltpu.SemaphoreType.DMA
    wide = GROUP * ROWS
    shapes = (
        jax.ShapeDtypeStruct((ROWS, 128), BF16),
        jax.ShapeDtypeStruct((4, CODES), F32),
        jax.ShapeDtypeStruct((4, 128), F32),
        jax.ShapeDtypeStruct((8, 128), F32),
        jax.ShapeDtypeStruct((8, 128), F32),
    )
    results = pl.pallas_call(
        kernel,
        out_shape=shapes,
        in_specs=[pl.BlockSpec(memory_space=pltpu.SMEM)] + [hbm] * 9,
        out_specs=(vmem,) * 5,
        scratch_shapes=[
            pltpu.VMEM((2, 128), jnp.int32),
            pltpu.VMEM((1, CODES), jnp.int32),
            pltpu.VMEM((1, CODES), jnp.int32),
            pltpu.VMEM((8, 128), F32),
            pltpu.VMEM((8, 128), F32),
            pltpu.VMEM((CODES, 1024), BF16),
            pltpu.VMEM((1024, 128), BF16),
            pltpu.VMEM((ROWS, 128), BF16),
            pltpu.VMEM((1, 128), F32),
            dma((9,)),
            pltpu.VMEM((GROUP, 2, 128), F32),
            pltpu.VMEM((GROUP, ROWS, 128), BF16),
            pltpu.VMEM((wide, CODES), BF16),
            pltpu.VMEM((wide, 128), F32),
            pltpu.VMEM((wide, 128), F32),
            pltpu.VMEM((wide, 128), BF16),
            pltpu.VMEM((GROUP, ROWS, 128), BF16),
            pltpu.VMEM((CODES, 128), BF16),
            pltpu.VMEM((128, 128), BF16),
            pltpu.VMEM((8, 128), F32),
            pltpu.VMEM((1024, 128), BF16),
            pltpu.VMEM((8, CODES), F32),
            pltpu.VMEM((2, 8, 128), F32),
            pltpu.VMEM((PEERS, 2, 128), F32),
            pltpu.VMEM((PEERS, 2, 128), F32),
            pltpu.VMEM((GROUP, 2, 128), F32),
            pltpu.VMEM((GROUP, 2, 128), F32),
            pltpu.VMEM((16, 2, 8, 256), BF16),
            pltpu.VMEM((PEERS, 8, 256), BF16),
            pltpu.VMEM((16, 2, 8, 384), BF16),
            pltpu.VMEM((PEERS, 8, 384), BF16),
        ]
        + [dma, dma((GROUP,))]
        + [dma] * 14,
        compiler_params=pltpu.CompilerParams(
            collective_id=0, has_side_effects=True, vmem_limit_bytes=48 << 20
        ),
    )(
        counts,
        *(
            pltpu.with_memory_space_constraint(array, pltpu.HBM)
            for array in (
                ids.reshape(2, 128),
                hash_scale.reshape(1, CODES),
                hash_shift.reshape(1, CODES),
                norm_gain.reshape(8, 128),
                norm_bias.reshape(8, 128),
                w_code,
                w_out,
                cotangent,
                out_bias.reshape(1, 128),
            )
        ),
    )
    emb, gcode, gout, ggain, gbias = pl.pallas_call(
        store_kernel,
        out_shape=shapes,
        in_specs=[vmem] * 5,
        out_specs=(hbm,) * 5,
        scratch_shapes=[dma((5,))],
        compiler_params=pltpu.CompilerParams(vmem_limit_bytes=4 << 20),
    )(*results)
    return emb, gcode, gout, ggain.reshape(1024), gbias.reshape(1024)


def solution(mesh):
    finer = Mesh(mesh.devices.reshape(8, 4, 4, 2), AXES)
    return jax.shard_map(
        per_device,
        mesh=finer,
        in_specs=(P(AXES), P(AXES), P(), P(), P(), P(), P(), P(), P(), P(AXES, None)),
        out_specs=(P(AXES, None), P(AXES, None), P(AXES, None), P(), P()),
        check_vma=False,
    )
```

```python
import functools

import jax
import jax.numpy as jnp
from jax import lax
from jax.experimental import pallas as pl
from jax.experimental.pallas import tpu as pltpu
from jax.sharding import Mesh
from jax.sharding import PartitionSpec as P

AXES = ("z", "x", "y", "c")
MESH = pl.DeviceIdType.MESH
F32 = jnp.float32
BF16 = jnp.bfloat16
MODULUS = 65521
EPSILON = 1e-05
MAGIC = 12582912.0
TOTAL = 16384.0
ROWS = 256
CODES = 512
GROUP = 8
PEERS = 32
FAR = sorted(
    ((dz, dx) for dz in range(8) for dx in range(4) if dz or dx),
    key=lambda o: (-min(o[0], 8 - o[0]) - min(o[1], 4 - o[1]), o),
)
NEAR = [(0, 0), (0, 1), (1, 0), (3, 0), (1, 1), (3, 1), (2, 0), (2, 1)]
BACK = [NEAR.index(((4 - dy) % 4, dc)) for dy, dc in NEAR]

NN = (((1,), (0,)), ((), ()))
NT = (((1,), (1,)), ((), ()))
TN = (((0,), (0,)), ((), ()))


def dot(a, b, dims=NN):
    return lax.dot_general(a, b, dims, preferred_element_type=F32)


def iota(shape, dim):
    return lax.broadcasted_iota(jnp.int32, shape, dim)


def parts(values):
    high = values.astype(BF16)
    rest = values - high.astype(F32)
    mid = rest.astype(BF16)
    low = (rest - mid.astype(F32)).astype(BF16)
    return high, mid, low


def exact_pick(values, onehot):
    high, mid, low = parts(values)
    return dot(high, onehot) + dot(mid, onehot) + dot(low, onehot)


def hidden_pick(q):
    i = iota((128, 1024), 0)
    h = iota((128, 1024), 1)
    return jnp.where(h == (i // 4) * 32 + q * 4 + i % 4, 1.0, 0.0).astype(BF16)


def lane_picks():
    lane = iota((128, 1024), 0)
    i = iota((128, 1024), 1)
    return jnp.where(lane == ((i % 16) // 4) * 32 + (i // 128) * 4 + i % 4, 1.0, 0.0).astype(BF16)


def lane_put(q):
    i = iota((128, 128), 0)
    lane = iota((128, 128), 1)
    return jnp.where(lane == ((i % 16) // 4) * 32 + q * 4 + i % 4, 1.0, 0.0).astype(BF16)


def mish_terms(val):
    u = jnp.exp(jnp.minimum(val, 20.0))
    n = u * (u + 2.0)
    r = 1.0 / (n + 2.0)
    return u, n, r


def kernel(
    count_ref, ids_hbm, scale_hbm, shift_hbm, gain_hbm, bias_hbm, wcode_hbm, wout_hbm, cot_hbm, obias_hbm,
    emb_ref, gcode_ref, gout_ref, ggain_ref, gbias_ref,
    ids_ref, scale_ref, shift_ref, gain_ref, bias_ref, wcode_ref, wout_ref, cot_ref, obias_ref, s_in,
    idf, delta, code, pre, gact, dval, act, wown, wout_own, vec, put, pick_all, mix, nat, own, share, met,
    st, st2, par, tot, p_send, p_recv, a_send, a_recv,
    s_sh, r_sh, s_id, r_id, s_dl, r_dl, s_st, r_st, s_p, r_p, s_par, r_par, s_st2, r_st2, s_a, r_a, s_tot, r_tot,
):
    z, x, y, c = (lax.axis_index(a) for a in AXES)
    q = y * 2 + c
    zx = z * 4 + x

    z_at = [lax.rem(z + d, 8) for d in range(8)]
    x_at = [lax.rem(x + d, 4) for d in range(4)]
    x_half = [t // 2 for t in x_at]
    x_odd = [lax.rem(t, 2) for t in x_at]
    far = [(z_at[dz], x_at[dx], y, c) for dz, dx in FAR]
    y_at = [lax.rem(y + d, 4) for d in range(4)]
    c_at = [c, 1 - c]
    near = [(z, x, y_at[dy], c_at[dc]) for dy, dc in NEAR]

    loads = [
        pltpu.make_async_copy(src, dst, s_in.at[i])
        for i, (src, dst) in enumerate(
            (
                (ids_hbm, ids_ref),
                (scale_hbm, scale_ref),
                (shift_hbm, shift_ref),
                (wcode_hbm, wcode_ref),
                (cot_hbm, cot_ref),
                (wout_hbm, wout_ref),
                (gain_hbm, gain_ref),
                (bias_hbm, bias_ref),
                (obias_hbm, obias_ref),
            )
        )
    ]
    for load in loads:
        load.start()

    barrier = pltpu.get_barrier_semaphore()

    for device in far + near[1:]:
        pl.semaphore_signal(barrier, inc=1, device_id=device, device_id_type=MESH)

    def send(src, dst, send_sem, recv_sem, device):
        pltpu.make_async_remote_copy(
            src, dst, send_sem, recv_sem, device_id=device, device_id_type=MESH
        ).start()

    def to_near(buf, send_sem, recv_sem):
        for device in near[1:]:
            send(buf.at[q], buf.at[q], send_sem, recv_sem, device)

    def to_far(buf, send_sem, recv_sem):
        for device in far:
            send(buf.at[zx], buf.at[zx], send_sem, recv_sem, device)

    def scatter_far(src, dst, send_sem, recv_sem):
        for (dz, dx), device in zip(FAR, far):
            send(src.at[z_at[dz] * 2 + x_half[dx], x_odd[dx]], dst.at[zx], send_sem, recv_sem, device)

    def wait(buf, n, sem):
        part = buf.at[pl.ds(0, n)]
        pltpu.make_async_copy(part, part, sem).wait()

    count = count_ref[0]
    loads[0].wait()
    slot = iota((2, 128), 0) * 128 + iota((2, 128), 1)
    idf[0] = jnp.where(slot < count, ids_ref[...].astype(F32), -1.0)
    for load in loads[1:3]:
        load.wait()
    scale = scale_ref[...].astype(F32)
    high = scale * 256.0
    high = high - ((high * (1.0 / MODULUS) + MAGIC) - MAGIC) * float(MODULUS)
    table = []
    for v in (high, scale, shift_ref[...].astype(F32)):
        coarse = jnp.floor(v * (1.0 / 256.0)) * 256.0
        table += [coarse, v - coarse]
    table = jnp.concatenate(table + [jnp.zeros((10, CODES), F32)], axis=0)
    flag = jnp.where(iota((16, 128), 0) == 6, 1.0, 0.0)
    mix[...] = jnp.concatenate([table, flag], axis=1).astype(BF16)

    def hash_rows(k):
        ident = jnp.concatenate([idf[k, 0:1, :], idf[k, 1:2, :]], axis=1)
        upper = jnp.floor(ident * (1.0 / 256.0))
        lower = ident - upper * 256.0
        alive = jnp.where(ident >= 0.0, 1.0, 0.0)
        row = iota((16, ROWS), 0)
        terms = jnp.where(row < 2, upper, jnp.where(row < 4, lower, jnp.where(row < 6, 1.0, jnp.where(row < 7, alive, 0.0))))
        mixed = dot(terms.astype(BF16), mix[...], TN)
        value = mixed[:, :CODES]
        times = (value * (1.0 / MODULUS) + MAGIC) - MAGIC
        bucket = value - times * float(MODULUS)
        bucket = jnp.where(bucket < 0.0, bucket + float(MODULUS), bucket)
        return bucket * (2.0 / (MODULUS - 1)) - 1.0, mixed[:, CODES:]

    def hash_other(k):
        rows, alive = hash_rows(k)
        rows = rows.astype(BF16)
        code[k * ROWS : k * ROWS + ROWS, :] = rows
        pre[k * ROWS : k * ROWS + ROWS, :] = dot(rows, wown[...]) * alive

    rows, alive = hash_rows(0)
    rows = (rows * jnp.concatenate([alive] * 4, axis=1)).astype(BF16)
    code[0:ROWS, :] = rows
    pick_all[...] = lane_picks()
    own_z = iota((8, 128), 0) == iota((8, 128), 1) // 16
    loads[3].wait()
    rows_of = []
    for k in range(GROUP):
        hidden = dot(rows, wcode_ref[:, k * 128 : k * 128 + 128])
        own[:, k * 128 : k * 128 + 128] = hidden
        rows_of.append((jnp.sum(hidden, axis=0, keepdims=True), jnp.sum(hidden * hidden, axis=0, keepdims=True)))
    by_z = jnp.concatenate([r[v] for v in range(2) for r in rows_of], axis=0)
    by_unit = dot(jnp.concatenate(parts(by_z), axis=0), pick_all[...])
    by_unit = by_unit[0:16] + by_unit[16:32] + by_unit[32:48]
    for k in range(GROUP):
        unit = by_unit[:, k * 128 : k * 128 + 128]
        share[k] = jnp.concatenate(
            [jnp.sum(jnp.where(own_z, unit[8 * v : 8 * v + 8], 0.0), axis=0, keepdims=True) for v in range(2)], axis=0
        )

    pl.semaphore_wait(barrier, PEERS - 1 + GROUP - 1)
    for k in range(1, GROUP):
        dy, dc = NEAR[k]
        send(share.at[y_at[dy] * 2 + c_at[dc]], met.at[BACK[k]], s_sh, r_sh, near[k])
    met[0] = share[q]
    for k in range(1, GROUP):
        send(idf.at[0], idf.at[BACK[k]], s_id, r_id.at[BACK[k]], near[k])

    loads[4].wait()
    live = iota((ROWS, 128), 0) < count
    delta[0] = jnp.where(live, cot_ref[...].astype(F32) * (1.0 / 128.0), 0.0).astype(BF16)
    for k in range(1, GROUP):
        send(delta.at[0], delta.at[BACK[k]], s_dl, r_dl, near[k])

    for load in loads[5:]:
        load.wait()
    pick = hidden_pick(q)
    wown[...] = dot(wcode_ref[...], pick, NT).astype(BF16)

    pre[0:ROWS, :] = dot(code[0:ROWS, :], wown[...])
    wout_own[...] = dot(pick, wout_ref[...]).astype(BF16)
    small = pick_all[:, pl.ds(pl.multiple_of(q * 128, 128), 128)]
    vec[0:1] = jnp.sum(jnp.where(own_z, exact_pick(gain_ref[...], small), 0.0), axis=0, keepdims=True)
    vec[1:2] = jnp.sum(jnp.where(own_z, exact_pick(bias_ref[...], small), 0.0), axis=0, keepdims=True)
    for b in range(GROUP):
        put[b * 128 : b * 128 + 128, :] = lane_put(b)
    pltpu.make_async_copy(idf.at[1], idf.at[1], r_id.at[1]).wait()
    hash_other(1)

    wait(met, GROUP - 1, r_sh)
    st[zx] = jnp.sum(met[...], axis=0)
    to_far(st, s_st, r_st)

    for batch in ((2, 3), (4, 5), (6, 7)):
        for k in batch:
            pltpu.make_async_copy(idf.at[k], idf.at[k], r_id.at[k]).wait()
        for k in batch:
            hash_other(k)

    def stacked(full, lo):
        tiles = full.reshape(16, 8, full.shape[1])
        part = tiles[:, lo : lo + 4, :]
        return jnp.concatenate([part[:, :, :256], part[:, :, 256:]], axis=1)

    p_full = dot(pre[...].astype(BF16), code[...], TN)
    for parity in range(2):
        p_send[:, parity] = stacked(p_full, parity * 4).astype(BF16)
    p_recv[zx] = p_send[zx // 2, lax.rem(zx, 2)]
    scatter_far(p_send, p_recv, s_p, r_p)
    alive = jnp.concatenate([jnp.where(idf[b, h : h + 1, :] >= 0.0, 1.0, 0.0) for b in range(8) for h in range(2)], axis=1)
    code_sum = dot(jnp.broadcast_to(alive, (8, GROUP * ROWS)).astype(BF16), code[...])[0:1]

    wait(delta, GROUP - 1, r_dl)

    for k in range(GROUP):
        gact[k * ROWS : k * ROWS + ROWS, :] = dot(delta[k], wout_own[...], NT)

    def in_order(ref):
        blocks = [
            jnp.concatenate([jnp.where(own_z, ref[b, v : v + 1, :], 0.0) for b in range(GROUP)], axis=1) for v in range(2)
        ]
        out = dot(jnp.concatenate(parts(jnp.concatenate(blocks, axis=0)), axis=0), put[...])
        return out[0:16] + out[16:32] + out[32:48]

    wait(st, PEERS - 1, r_st)
    moments = jnp.sum(st[...], axis=0) * (1.0 / TOTAL)
    mean = moments[0:1]
    inv_std = lax.rsqrt(moments[1:2] - mean * mean + EPSILON)
    gain = vec[0:1]
    bias = vec[1:2]
    par[q] = jnp.concatenate([mean, inv_std], axis=0)
    to_near(par, s_par, r_par)

    def second(b, carry):
        sum_gain, sum_bias = carry
        at = pl.multiple_of(b * ROWS, ROWS)
        normed = (pre[pl.ds(at, ROWS), :] - mean) * inv_std
        val = normed * gain + bias
        u, n, r = mish_terms(val)
        act[b] = (val * (n * r)).astype(BF16)
        slope = r * (n + 4.0 * val * (u * (1.0 + u)) * r)
        d = gact[pl.ds(at, ROWS), :] * slope
        dval[pl.ds(at, ROWS), :] = d.astype(BF16)
        return (
            sum_gain + jnp.sum(d * normed, axis=0, keepdims=True),
            sum_bias + jnp.sum(d, axis=0, keepdims=True),
        )

    zero = jnp.zeros((1, 128), F32)
    sums = lax.fori_loop(0, GROUP, second, (zero, zero))
    st2[zx] = jnp.concatenate(sums, axis=0)
    to_far(st2, s_st2, r_st2)

    a_full = dot(dval[...], code[...], TN)
    o_full = dot(act[...].reshape(GROUP * ROWS, 128), delta[...].reshape(GROUP * ROWS, 128), TN)
    s_rows = jnp.concatenate([code_sum[:, 128 * i : 128 * i + 128] for i in range(4)], axis=0)
    s_tiles = jnp.broadcast_to(s_rows[None], (16, 4, 128))
    o_tiles = o_full.reshape(16, 8, 128)
    for parity in range(2):
        a_send[:, parity, :, 0:256] = stacked(a_full, parity * 4).astype(BF16)
        both = jnp.concatenate([o_tiles[:, parity * 4 : parity * 4 + 4, :], s_tiles], axis=1)
        a_send[:, parity, :, 256:384] = both.astype(BF16)
    a_recv[zx] = a_send[zx // 2, lax.rem(zx, 2)]
    scatter_far(a_send, a_recv, s_a, r_a)

    wait(par, GROUP - 1, r_par)
    ordered = in_order(par)
    nat[0] = ordered[0:8]
    nat[1] = ordered[8:16] * gain_ref[...]

    acc = jnp.zeros((ROWS, 128), F32)
    for k in range(GROUP):
        hidden = own[:, k * 128 : k * 128 + 128]
        val = (hidden - nat[0, k : k + 1, :]) * nat[1, k : k + 1, :] + bias_ref[k : k + 1, :]
        _, n, r = mish_terms(val)
        acc = acc + dot((val * (n * r)).astype(BF16), wout_ref[k * 128 : k * 128 + 128, :])
    live = iota((ROWS, 128), 0) < count
    emb_ref[...] = jnp.where(live, acc + obias_ref[...], 0.0).astype(BF16)

    wait(st2, PEERS - 1, r_st2)
    sums = jnp.sum(st2[...], axis=0)
    tot[q] = sums
    to_near(tot, s_tot, r_tot)

    k1 = inv_std * gain
    k3 = k1 * inv_std * sums[0:1] * (1.0 / TOTAL)
    k2 = k1 * sums[1:2] * (1.0 / TOTAL) - k3 * mean
    mine = iota((8, 128), 1) == zx * 4 + iota((8, 128), 0) % 4

    def column(v):
        return jnp.sum(jnp.where(mine, v, 0.0), axis=1, keepdims=True)

    wait(p_recv, PEERS - 1, r_p)
    p_sum = jnp.sum(p_recv[...].astype(F32), axis=0)
    wait(a_recv, PEERS - 1, r_a)
    a_sum = jnp.sum(a_recv[...].astype(F32), axis=0)
    s_all = a_sum[4:8, 256:384]
    upper = jnp.concatenate([s_all[0:1], s_all[1:2]], axis=1)
    lower = jnp.concatenate([s_all[2:3], s_all[3:4]], axis=1)
    s_both = jnp.where(iota((8, 256), 0) < 4, upper, lower)
    grad = column(k1) * a_sum[:, 0:256] - column(k2) * s_both - column(k3) * p_sum
    gcode_ref[...] = jnp.concatenate([grad[0:4], grad[4:8]], axis=1)
    gout_ref[...] = a_sum[0:4, 256:384]

    wait(tot, GROUP - 1, r_tot)
    ordered = in_order(tot)
    ggain_ref[...] = ordered[0:8]
    gbias_ref[...] = ordered[8:16]

    wait(met, GROUP - 1, s_sh)
    wait(idf, GROUP - 1, s_id)
    wait(delta, GROUP - 1, s_dl)
    wait(st, PEERS - 1, s_st)
    wait(p_recv, PEERS - 1, s_p)
    wait(par, GROUP - 1, s_par)
    wait(st2, PEERS - 1, s_st2)
    wait(a_recv, PEERS - 1, s_a)
    wait(tot, GROUP - 1, s_tot)


def store_kernel(*refs):
    srcs, dsts, sem = refs[:5], refs[5:10], refs[10]
    copies = [pltpu.make_async_copy(a, b, sem.at[i]) for i, (a, b) in enumerate(zip(srcs, dsts))]
    for copy in copies:
        copy.start()
    for copy in copies:
        copy.wait()


def per_device(ids, counts, hash_scale, hash_shift, w_code, norm_gain, norm_bias, w_out, out_bias, cotangent):
    vmem = pl.BlockSpec(memory_space=pltpu.VMEM)
    hbm = pl.BlockSpec(memory_space=pltpu.HBM)
    dma = pltpu.SemaphoreType.DMA
    wide = GROUP * ROWS
    shapes = (
        jax.ShapeDtypeStruct((ROWS, 128), BF16),
        jax.ShapeDtypeStruct((4, CODES), F32),
        jax.ShapeDtypeStruct((4, 128), F32),
        jax.ShapeDtypeStruct((8, 128), F32),
        jax.ShapeDtypeStruct((8, 128), F32),
    )
    results = pl.pallas_call(
        kernel,
        out_shape=shapes,
        in_specs=[pl.BlockSpec(memory_space=pltpu.SMEM)] + [hbm] * 9,
        out_specs=(vmem,) * 5,
        scratch_shapes=[
            pltpu.VMEM((2, 128), jnp.int32),
            pltpu.VMEM((1, CODES), jnp.int32),
            pltpu.VMEM((1, CODES), jnp.int32),
            pltpu.VMEM((8, 128), F32),
            pltpu.VMEM((8, 128), F32),
            pltpu.VMEM((CODES, 1024), BF16),
            pltpu.VMEM((1024, 128), BF16),
            pltpu.VMEM((ROWS, 128), BF16),
            pltpu.VMEM((1, 128), F32),
            dma((9,)),
            pltpu.VMEM((GROUP, 2, 128), F32),
            pltpu.VMEM((GROUP, ROWS, 128), BF16),
            pltpu.VMEM((wide, CODES), BF16),
            pltpu.VMEM((wide, 128), F32),
            pltpu.VMEM((wide, 128), F32),
            pltpu.VMEM((wide, 128), BF16),
            pltpu.VMEM((GROUP, ROWS, 128), BF16),
            pltpu.VMEM((CODES, 128), BF16),
            pltpu.VMEM((128, 128), BF16),
            pltpu.VMEM((8, 128), F32),
            pltpu.VMEM((1024, 128), BF16),
            pltpu.VMEM((128, 1024), BF16),
            pltpu.VMEM((16, CODES + 128), BF16),
            pltpu.VMEM((2, 8, 128), F32),
            pltpu.VMEM((ROWS, 1024), F32),
            pltpu.VMEM((GROUP, 2, 128), F32),
            pltpu.VMEM((GROUP, 2, 128), F32),
            pltpu.VMEM((PEERS, 2, 128), F32),
            pltpu.VMEM((PEERS, 2, 128), F32),
            pltpu.VMEM((GROUP, 2, 128), F32),
            pltpu.VMEM((GROUP, 2, 128), F32),
            pltpu.VMEM((16, 2, 8, 256), BF16),
            pltpu.VMEM((PEERS, 8, 256), BF16),
            pltpu.VMEM((16, 2, 8, 384), BF16),
            pltpu.VMEM((PEERS, 8, 384), BF16),
        ]
        + [dma, dma, dma, dma((GROUP,))]
        + [dma] * 14,
        compiler_params=pltpu.CompilerParams(
            collective_id=0, has_side_effects=True, vmem_limit_bytes=48 << 20
        ),
    )(
        counts,
        *(
            pltpu.with_memory_space_constraint(array, pltpu.HBM)
            for array in (
                ids.reshape(2, 128),
                hash_scale.reshape(1, CODES),
                hash_shift.reshape(1, CODES),
                norm_gain.reshape(8, 128),
                norm_bias.reshape(8, 128),
                w_code,
                w_out,
                cotangent,
                out_bias.reshape(1, 128),
            )
        ),
    )
    emb, gcode, gout, ggain, gbias = pl.pallas_call(
        store_kernel,
        out_shape=shapes,
        in_specs=[vmem] * 5,
        out_specs=(hbm,) * 5,
        scratch_shapes=[dma((5,))],
        compiler_params=pltpu.CompilerParams(vmem_limit_bytes=4 << 20),
    )(*results)
    return emb, gcode, gout, ggain.reshape(1024), gbias.reshape(1024)


def solution(mesh):
    finer = Mesh(mesh.devices.reshape(8, 4, 4, 2), AXES)
    return jax.shard_map(
        per_device,
        mesh=finer,
        in_specs=(P(AXES), P(AXES), P(), P(), P(), P(), P(), P(), P(), P(AXES, None)),
        out_specs=(P(AXES, None), P(AXES, None), P(AXES, None), P(), P()),
        check_vma=False,
    )
```

```python
import functools

import jax
import jax.numpy as jnp
from jax import lax
from jax.experimental import pallas as pl
from jax.experimental.pallas import tpu as pltpu
from jax.sharding import Mesh
from jax.sharding import PartitionSpec as P

AXES = ("z", "x", "y", "c")
MESH = pl.DeviceIdType.MESH
F32 = jnp.float32
BF16 = jnp.bfloat16
MODULUS = 65521
EPSILON = 1e-05
MAGIC = 12582912.0
TOTAL = 16384.0
ROWS = 256
CODES = 512
GROUP = 8
PEERS = 32
FAR = sorted(
    ((dz, dx) for dz in range(8) for dx in range(4) if dz or dx),
    key=lambda o: (-min(o[0], 8 - o[0]) - min(o[1], 4 - o[1]), o),
)
NEAR = [(0, 0), (0, 1), (1, 0), (3, 0), (1, 1), (3, 1), (2, 0), (2, 1)]
BACK = [NEAR.index(((4 - dy) % 4, dc)) for dy, dc in NEAR]

NN = (((1,), (0,)), ((), ()))
NT = (((1,), (1,)), ((), ()))
TN = (((0,), (0,)), ((), ()))


def dot(a, b, dims=NN):
    return lax.dot_general(a, b, dims, preferred_element_type=F32)


def iota(shape, dim):
    return lax.broadcasted_iota(jnp.int32, shape, dim)


def parts(values):
    high = values.astype(BF16)
    rest = values - high.astype(F32)
    mid = rest.astype(BF16)
    low = (rest - mid.astype(F32)).astype(BF16)
    return high, mid, low


def exact_pick(values, onehot):
    high, mid, low = parts(values)
    return dot(high, onehot) + dot(mid, onehot) + dot(low, onehot)


def hidden_pick(q):
    i = iota((128, 1024), 0)
    h = iota((128, 1024), 1)
    return jnp.where(h == (i // 4) * 32 + q * 4 + i % 4, 1.0, 0.0).astype(BF16)


def lane_picks():
    lane = iota((128, 1024), 0)
    i = iota((128, 1024), 1)
    return jnp.where(lane == ((i % 16) // 4) * 32 + (i // 128) * 4 + i % 4, 1.0, 0.0).astype(BF16)


def lane_put(q):
    i = iota((128, 128), 0)
    lane = iota((128, 128), 1)
    return jnp.where(lane == ((i % 16) // 4) * 32 + q * 4 + i % 4, 1.0, 0.0).astype(BF16)


def mish_terms(val):
    u = jnp.exp(jnp.minimum(val, 20.0))
    n = u * (u + 2.0)
    r = 1.0 / (n + 2.0)
    return u, n, r


def kernel(
    count_ref, ids_hbm, scale_hbm, shift_hbm, gain_hbm, bias_hbm, wcode_hbm, wout_hbm, cot_hbm, obias_hbm,
    emb_ref, gcode_ref, gout_ref, ggain_ref, gbias_ref,
    ids_ref, scale_ref, shift_ref, gain_ref, bias_ref, wcode_ref, wout_ref, cot_ref, obias_ref, s_in,
    idf, delta, code, pre, gact, dval, act, wown, wout_own, vec, put, pick_all, mix, nat, own, share, met,
    st_out, st, st2_own, st2, par, tot, p_send, p_recv, a_send, a_recv,
    s_sh, r_sh, s_id, r_id, s_dl, r_dl, s_st, r_st, s_p, r_p, s_par, r_par, s_st2, r_st2, s_a, r_a, s_tot, r_tot,
):
    z, x, y, c = (lax.axis_index(a) for a in AXES)
    q = y * 2 + c
    zx = z * 4 + x

    z_at = [lax.rem(z + d, 8) for d in range(8)]
    x_at = [lax.rem(x + d, 4) for d in range(4)]
    x_half = [t // 2 for t in x_at]
    x_odd = [lax.rem(t, 2) for t in x_at]
    far = [(z_at[dz], x_at[dx], y, c) for dz, dx in FAR]
    across = [(z_at[dz], x_at[dx], y, 1 - c) for dz, dx in FAR]
    far_zero = [(z_at[dz], x_at[dx], y, 0) for dz, dx in FAR]
    far_hub = [(z_at[dz], x_at[dx], y, 1) for dz, dx in FAR]
    hub = c == 1
    y_at = [lax.rem(y + d, 4) for d in range(4)]
    c_at = [c, 1 - c]
    near = [(z, x, y_at[dy], c_at[dc]) for dy, dc in NEAR]

    loads = [
        pltpu.make_async_copy(src, dst, s_in.at[i])
        for i, (src, dst) in enumerate(
            (
                (ids_hbm, ids_ref),
                (scale_hbm, scale_ref),
                (shift_hbm, shift_ref),
                (wcode_hbm, wcode_ref),
                (cot_hbm, cot_ref),
                (wout_hbm, wout_ref),
                (gain_hbm, gain_ref),
                (bias_hbm, bias_ref),
                (obias_hbm, obias_ref),
            )
        )
    ]
    for load in loads:
        load.start()

    barrier = pltpu.get_barrier_semaphore()

    for device in far + across + near[1:]:
        pl.semaphore_signal(barrier, inc=1, device_id=device, device_id_type=MESH)

    def send(src, dst, send_sem, recv_sem, device):
        pltpu.make_async_remote_copy(
            src, dst, send_sem, recv_sem, device_id=device, device_id_type=MESH
        ).start()

    def to_near(buf, send_sem, recv_sem):
        for device in near[1:]:
            send(buf.at[q], buf.at[q], send_sem, recv_sem, device)

    def scatter_far(src, dst, send_sem, recv_sem):
        for (dz, dx), device in zip(FAR, far):
            send(src.at[z_at[dz] * 2 + x_half[dx], x_odd[dx]], dst.at[zx], send_sem, recv_sem, device)

    def wait(buf, n, sem):
        part = buf.at[pl.ds(0, n)]
        pltpu.make_async_copy(part, part, sem).wait()

    count = count_ref[0]
    loads[0].wait()
    slot = iota((2, 128), 0) * 128 + iota((2, 128), 1)
    idf[0] = jnp.where(slot < count, ids_ref[...].astype(F32), -1.0)
    for load in loads[1:3]:
        load.wait()
    scale = scale_ref[...].astype(F32)
    high = scale * 256.0
    high = high - ((high * (1.0 / MODULUS) + MAGIC) - MAGIC) * float(MODULUS)
    table = []
    for v in (high, scale, shift_ref[...].astype(F32)):
        coarse = jnp.floor(v * (1.0 / 256.0)) * 256.0
        table += [coarse, v - coarse]
    table = jnp.concatenate(table + [jnp.zeros((10, CODES), F32)], axis=0)
    flag = jnp.where(iota((16, 128), 0) == 6, 1.0, 0.0)
    mix[...] = jnp.concatenate([table, flag], axis=1).astype(BF16)

    def hash_rows(k):
        ident = jnp.concatenate([idf[k, 0:1, :], idf[k, 1:2, :]], axis=1)
        upper = jnp.floor(ident * (1.0 / 256.0))
        lower = ident - upper * 256.0
        alive = jnp.where(ident >= 0.0, 1.0, 0.0)
        row = iota((16, ROWS), 0)
        terms = jnp.where(row < 2, upper, jnp.where(row < 4, lower, jnp.where(row < 6, 1.0, jnp.where(row < 7, alive, 0.0))))
        mixed = dot(terms.astype(BF16), mix[...], TN)
        value = mixed[:, :CODES]
        times = (value * (1.0 / MODULUS) + MAGIC) - MAGIC
        bucket = value - times * float(MODULUS)
        bucket = jnp.where(bucket < 0.0, bucket + float(MODULUS), bucket)
        return bucket * (2.0 / (MODULUS - 1)) - 1.0, mixed[:, CODES:]

    def hash_other(k):
        rows, alive = hash_rows(k)
        rows = rows.astype(BF16)
        code[k * ROWS : k * ROWS + ROWS, :] = rows
        pre[k * ROWS : k * ROWS + ROWS, :] = dot(rows, wown[...]) * alive

    rows, alive = hash_rows(0)
    rows = (rows * jnp.concatenate([alive] * 4, axis=1)).astype(BF16)
    code[0:ROWS, :] = rows
    pick_all[...] = lane_picks()
    own_z = iota((8, 128), 0) == iota((8, 128), 1) // 16
    loads[3].wait()
    rows_of = []
    for k in range(GROUP):
        hidden = dot(rows, wcode_ref[:, k * 128 : k * 128 + 128])
        own[:, k * 128 : k * 128 + 128] = hidden
        rows_of.append((jnp.sum(hidden, axis=0, keepdims=True), jnp.sum(hidden * hidden, axis=0, keepdims=True)))
    by_z = jnp.concatenate([r[v] for v in range(2) for r in rows_of], axis=0)
    by_unit = dot(jnp.concatenate(parts(by_z), axis=0), pick_all[...])
    by_unit = by_unit[0:16] + by_unit[16:32] + by_unit[32:48]
    for k in range(GROUP):
        unit = by_unit[:, k * 128 : k * 128 + 128]
        share[k // 2, k % 2] = jnp.concatenate(
            [jnp.sum(jnp.where(own_z, unit[8 * v : 8 * v + 8], 0.0), axis=0, keepdims=True) for v in range(2)], axis=0
        )

    pl.semaphore_wait(barrier, 2 * (PEERS - 1) + GROUP - 1)
    for dy in (2, 1, 3):
        send(share.at[y_at[dy]], met.at[(4 - dy) * 2 + 1 - c], s_sh, r_sh, (z, x, y_at[dy], 1))

    @pl.when(hub)
    def _():
        met[0] = share[y]

    @pl.when(c == 0)
    def _():
        send(share.at[y], met.at[1], s_sh, r_sh, (z, x, y, 1))

    for k in range(1, GROUP):
        send(idf.at[0], idf.at[BACK[k]], s_id, r_id.at[BACK[k]], near[k])

    loads[4].wait()
    live = iota((ROWS, 128), 0) < count
    delta[0] = jnp.where(live, cot_ref[...].astype(F32) * (1.0 / 128.0), 0.0).astype(BF16)
    for k in range(1, GROUP):
        send(delta.at[0], delta.at[BACK[k]], s_dl, r_dl, near[k])

    for load in loads[5:]:
        load.wait()
    pick = hidden_pick(q)
    wown[...] = dot(wcode_ref[...], pick, NT).astype(BF16)

    pre[0:ROWS, :] = dot(code[0:ROWS, :], wown[...])
    wout_own[...] = dot(pick, wout_ref[...]).astype(BF16)
    small = pick_all[:, pl.ds(pl.multiple_of(q * 128, 128), 128)]
    vec[0:1] = jnp.sum(jnp.where(own_z, exact_pick(gain_ref[...], small), 0.0), axis=0, keepdims=True)
    vec[1:2] = jnp.sum(jnp.where(own_z, exact_pick(bias_ref[...], small), 0.0), axis=0, keepdims=True)
    for b in range(GROUP):
        put[b * 128 : b * 128 + 128, :] = lane_put(b)
    pltpu.make_async_copy(idf.at[1], idf.at[1], r_id.at[1]).wait()
    hash_other(1)

    @pl.when(hub)
    def _():
        wait(met, GROUP - 1, r_sh)
        both = jnp.sum(met[...], axis=0)
        st_out[...] = both
        st[zx] = both[1]
        for zero, one in zip(far_zero, far_hub):
            send(st_out.at[0], st.at[zx], s_st, r_st, zero)
            send(st_out.at[1], st.at[zx], s_st, r_st, one)
        send(st_out.at[0], st.at[zx], s_st, r_st, (z, x, y, 0))

    for batch in ((2, 3), (4, 5), (6, 7)):
        for k in batch:
            pltpu.make_async_copy(idf.at[k], idf.at[k], r_id.at[k]).wait()
        for k in batch:
            hash_other(k)

    def stacked(full, lo):
        tiles = full.reshape(16, 8, full.shape[1])
        part = tiles[:, lo : lo + 4, :]
        return jnp.concatenate([part[:, :, :256], part[:, :, 256:]], axis=1)

    p_full = dot(pre[...].astype(BF16), code[...], TN)
    for parity in range(2):
        p_send[:, parity] = stacked(p_full, parity * 4).astype(BF16)
    p_recv[zx] = p_send[zx // 2, lax.rem(zx, 2)]
    scatter_far(p_send, p_recv, s_p, r_p)
    alive = jnp.concatenate([jnp.where(idf[b, h : h + 1, :] >= 0.0, 1.0, 0.0) for b in range(8) for h in range(2)], axis=1)
    code_sum = dot(jnp.broadcast_to(alive, (8, GROUP * ROWS)).astype(BF16), code[...])[0:1]

    wait(delta, GROUP - 1, r_dl)

    for k in range(GROUP):
        gact[k * ROWS : k * ROWS + ROWS, :] = dot(delta[k], wout_own[...], NT)

    def in_order(row):
        blocks = [jnp.concatenate([jnp.where(own_z, row(b, v), 0.0) for b in range(GROUP)], axis=1) for v in range(2)]
        out = dot(jnp.concatenate(parts(jnp.concatenate(blocks, axis=0)), axis=0), put[...])
        return out[0:16] + out[16:32] + out[32:48]

    @pl.when(hub)
    def _():
        wait(st, PEERS - 1, r_st)

    @pl.when(c == 0)
    def _():
        wait(st, PEERS, r_st)

    moments = jnp.sum(st[...], axis=0) * (1.0 / TOTAL)
    mean = moments[0:1]
    inv_std = lax.rsqrt(moments[1:2] - mean * mean + EPSILON)
    gain = vec[0:1]
    bias = vec[1:2]
    par[q] = jnp.concatenate([mean, inv_std], axis=0)
    to_near(par, s_par, r_par)

    slope_in = inv_std * gain

    def second(b, carry):
        sum_gain, sum_bias = carry
        at = pl.multiple_of(b * ROWS, ROWS)
        centred = pre[pl.ds(at, ROWS), :] - mean
        val = centred * slope_in + bias
        u, n, r = mish_terms(val)
        ratio = val * r
        act[b] = (n * ratio).astype(BF16)
        slope = r * (n + 4.0 * ((n - u) * ratio))
        d = gact[pl.ds(at, ROWS), :] * slope
        dval[pl.ds(at, ROWS), :] = d.astype(BF16)
        return (
            sum_gain + jnp.sum(d * centred, axis=0, keepdims=True),
            sum_bias + jnp.sum(d, axis=0, keepdims=True),
        )

    zero = jnp.zeros((1, 128), F32)
    sums = lax.fori_loop(0, GROUP, second, (zero, zero))
    mine2 = jnp.concatenate([sums[0] * inv_std, sums[1]], axis=0)
    st2_own[...] = mine2
    for one in far_hub:
        send(st2_own, st2.at[c * PEERS + zx], s_st2, r_st2, one)

    @pl.when(hub)
    def _():
        st2[PEERS + zx] = mine2

    @pl.when(c == 0)
    def _():
        send(st2_own, st2.at[zx], s_st2, r_st2, (z, x, y, 1))


    a_full = dot(dval[...], code[...], TN)
    o_full = dot(act[...].reshape(GROUP * ROWS, 128), delta[...].reshape(GROUP * ROWS, 128), TN)
    s_rows = jnp.concatenate([code_sum[:, 128 * i : 128 * i + 128] for i in range(4)], axis=0)
    s_tiles = jnp.broadcast_to(s_rows[None], (16, 4, 128))
    o_tiles = o_full.reshape(16, 8, 128)
    for parity in range(2):
        a_send[:, parity, :, 0:256] = stacked(a_full, parity * 4).astype(BF16)
        both = jnp.concatenate([o_tiles[:, parity * 4 : parity * 4 + 4, :], s_tiles], axis=1)
        a_send[:, parity, :, 256:384] = both.astype(BF16)
    a_recv[zx] = a_send[zx // 2, lax.rem(zx, 2)]
    scatter_far(a_send, a_recv, s_a, r_a)

    wait(par, GROUP - 1, r_par)
    ordered = in_order(lambda b, v: par[b, v : v + 1, :])
    nat[0] = ordered[0:8]
    nat[1] = ordered[8:16] * gain_ref[...]

    acc = jnp.zeros((ROWS, 128), F32)
    for k in range(GROUP):
        hidden = own[:, k * 128 : k * 128 + 128]
        val = (hidden - nat[0, k : k + 1, :]) * nat[1, k : k + 1, :] + bias_ref[k : k + 1, :]
        _, n, r = mish_terms(val)
        acc = acc + dot((n * (val * r)).astype(BF16), wout_ref[k * 128 : k * 128 + 128, :])
    live = iota((ROWS, 128), 0) < count
    emb_ref[...] = jnp.where(live, acc + obias_ref[...], 0.0).astype(BF16)

    @pl.when(hub)
    def _():
        wait(st2, 2 * PEERS - 1, r_st2)
        for v in range(2):
            tot[y, v] = jnp.sum(st2[v * PEERS : v * PEERS + PEERS], axis=0)
        for dy in (2, 1, 3):
            for core in (0, 1):
                send(tot.at[y], tot.at[y], s_tot, r_tot, (z, x, y_at[dy], core))
        send(tot.at[y], tot.at[y], s_tot, r_tot, (z, x, y, 0))

    wait(p_recv, PEERS - 1, r_p)
    p_sum = jnp.sum(p_recv[...].astype(F32), axis=0)
    wait(a_recv, PEERS - 1, r_a)
    a_sum = jnp.sum(a_recv[...].astype(F32), axis=0)
    gout_ref[...] = a_sum[0:4, 256:384]

    @pl.when(hub)
    def _():
        wait(tot, 3, r_tot)

    @pl.when(c == 0)
    def _():
        wait(tot, 4, r_tot)

    ordered = in_order(lambda b, v: tot[b // 2, b % 2, v : v + 1, :])
    ggain_ref[...] = ordered[0:8]
    gbias_ref[...] = ordered[8:16]

    sums = tot[y, c]
    k1 = inv_std * gain
    k3 = k1 * inv_std * sums[0:1] * (1.0 / TOTAL)
    k2 = k1 * sums[1:2] * (1.0 / TOTAL) - k3 * mean
    mine = iota((8, 128), 1) == zx * 4 + iota((8, 128), 0) % 4

    def column(v):
        return jnp.sum(jnp.where(mine, v, 0.0), axis=1, keepdims=True)

    s_all = a_sum[4:8, 256:384]
    upper = jnp.concatenate([s_all[0:1], s_all[1:2]], axis=1)
    lower = jnp.concatenate([s_all[2:3], s_all[3:4]], axis=1)
    s_both = jnp.where(iota((8, 256), 0) < 4, upper, lower)
    grad = column(k1) * a_sum[:, 0:256] - column(k2) * s_both - column(k3) * p_sum
    gcode_ref[...] = jnp.concatenate([grad[0:4], grad[4:8]], axis=1)

    @pl.when(hub)
    def _():
        wait(met, 3, s_sh)
        wait(st2, 2 * PEERS - 1, s_st)
        wait(st2, PEERS - 1, s_st2)
        wait(met, GROUP - 1, s_tot)

    @pl.when(c == 0)
    def _():
        wait(met, 4, s_sh)
        wait(st2, PEERS, s_st2)

    wait(idf, GROUP - 1, s_id)
    wait(delta, GROUP - 1, s_dl)
    wait(p_recv, PEERS - 1, s_p)
    wait(par, GROUP - 1, s_par)
    wait(a_recv, PEERS - 1, s_a)


def store_kernel(*refs):
    srcs, dsts, sem = refs[:5], refs[5:10], refs[10]
    copies = [pltpu.make_async_copy(a, b, sem.at[i]) for i, (a, b) in enumerate(zip(srcs, dsts))]
    for copy in copies:
        copy.start()
    for copy in copies:
        copy.wait()


def per_device(ids, counts, hash_scale, hash_shift, w_code, norm_gain, norm_bias, w_out, out_bias, cotangent):
    vmem = pl.BlockSpec(memory_space=pltpu.VMEM)
    hbm = pl.BlockSpec(memory_space=pltpu.HBM)
    dma = pltpu.SemaphoreType.DMA
    wide = GROUP * ROWS
    shapes = (
        jax.ShapeDtypeStruct((ROWS, 128), BF16),
        jax.ShapeDtypeStruct((4, CODES), F32),
        jax.ShapeDtypeStruct((4, 128), F32),
        jax.ShapeDtypeStruct((8, 128), F32),
        jax.ShapeDtypeStruct((8, 128), F32),
    )
    results = pl.pallas_call(
        kernel,
        out_shape=shapes,
        in_specs=[pl.BlockSpec(memory_space=pltpu.SMEM)] + [hbm] * 9,
        out_specs=(vmem,) * 5,
        scratch_shapes=[
            pltpu.VMEM((2, 128), jnp.int32),
            pltpu.VMEM((1, CODES), jnp.int32),
            pltpu.VMEM((1, CODES), jnp.int32),
            pltpu.VMEM((8, 128), F32),
            pltpu.VMEM((8, 128), F32),
            pltpu.VMEM((CODES, 1024), BF16),
            pltpu.VMEM((1024, 128), BF16),
            pltpu.VMEM((ROWS, 128), BF16),
            pltpu.VMEM((1, 128), F32),
            dma((9,)),
            pltpu.VMEM((GROUP, 2, 128), F32),
            pltpu.VMEM((GROUP, ROWS, 128), BF16),
            pltpu.VMEM((wide, CODES), BF16),
            pltpu.VMEM((wide, 128), F32),
            pltpu.VMEM((wide, 128), F32),
            pltpu.VMEM((wide, 128), BF16),
            pltpu.VMEM((GROUP, ROWS, 128), BF16),
            pltpu.VMEM((CODES, 128), BF16),
            pltpu.VMEM((128, 128), BF16),
            pltpu.VMEM((8, 128), F32),
            pltpu.VMEM((1024, 128), BF16),
            pltpu.VMEM((128, 1024), BF16),
            pltpu.VMEM((16, CODES + 128), BF16),
            pltpu.VMEM((2, 8, 128), F32),
            pltpu.VMEM((ROWS, 1024), F32),
            pltpu.VMEM((4, 2, 2, 128), F32),
            pltpu.VMEM((GROUP, 2, 2, 128), F32),
            pltpu.VMEM((2, 2, 128), F32),
            pltpu.VMEM((PEERS, 2, 128), F32),
            pltpu.VMEM((2, 128), F32),
            pltpu.VMEM((2 * PEERS, 2, 128), F32),
            pltpu.VMEM((GROUP, 2, 128), F32),
            pltpu.VMEM((4, 2, 2, 128), F32),
            pltpu.VMEM((16, 2, 8, 256), BF16),
            pltpu.VMEM((PEERS, 8, 256), BF16),
            pltpu.VMEM((16, 2, 8, 384), BF16),
            pltpu.VMEM((PEERS, 8, 384), BF16),
        ]
        + [dma, dma, dma, dma((GROUP,))]
        + [dma] * 14,
        compiler_params=pltpu.CompilerParams(
            collective_id=0, has_side_effects=True, vmem_limit_bytes=48 << 20
        ),
    )(
        counts,
        *(
            pltpu.with_memory_space_constraint(array, pltpu.HBM)
            for array in (
                ids.reshape(2, 128),
                hash_scale.reshape(1, CODES),
                hash_shift.reshape(1, CODES),
                norm_gain.reshape(8, 128),
                norm_bias.reshape(8, 128),
                w_code,
                w_out,
                cotangent,
                out_bias.reshape(1, 128),
            )
        ),
    )
    emb, gcode, gout, ggain, gbias = pl.pallas_call(
        store_kernel,
        out_shape=shapes,
        in_specs=[vmem] * 5,
        out_specs=(hbm,) * 5,
        scratch_shapes=[dma((5,))],
        compiler_params=pltpu.CompilerParams(vmem_limit_bytes=4 << 20),
    )(*results)
    return emb, gcode, gout, ggain.reshape(1024), gbias.reshape(1024)


def solution(mesh):
    finer = Mesh(mesh.devices.reshape(8, 4, 4, 2), AXES)
    return jax.shard_map(
        per_device,
        mesh=finer,
        in_specs=(P(AXES), P(AXES), P(), P(), P(), P(), P(), P(), P(), P(AXES, None)),
        out_specs=(P(AXES, None), P(AXES, None), P(AXES, None), P(), P()),
        check_vma=False,
    )
```

```python
import functools

import jax
import jax.numpy as jnp
from jax import lax
from jax.experimental import pallas as pl
from jax.experimental.pallas import tpu as pltpu
from jax.sharding import Mesh
from jax.sharding import PartitionSpec as P

AXES = ("z", "x", "y", "c")
MESH = pl.DeviceIdType.MESH
F32 = jnp.float32
BF16 = jnp.bfloat16
MODULUS = 65521
EPSILON = 1e-05
MAGIC = 12582912.0
TOTAL = 16384.0
ROWS = 256
CODES = 512
GROUP = 8
PEERS = 32
FAR = sorted(
    ((dz, dx) for dz in range(8) for dx in range(4) if dz or dx),
    key=lambda o: (-min(o[0], 8 - o[0]) - min(o[1], 4 - o[1]), o),
)
NEAR = [(0, 0), (0, 1), (1, 0), (3, 0), (1, 1), (3, 1), (2, 0), (2, 1)]
ACROSS = {k: NEAR.index((NEAR[k][0], 1)) for k in (2, 3, 6)}
BACK = [NEAR.index(((4 - dy) % 4, dc)) for dy, dc in NEAR]

NN = (((1,), (0,)), ((), ()))
NT = (((1,), (1,)), ((), ()))
TN = (((0,), (0,)), ((), ()))


def dot(a, b, dims=NN):
    return lax.dot_general(a, b, dims, preferred_element_type=F32)


def iota(shape, dim):
    return lax.broadcasted_iota(jnp.int32, shape, dim)


def parts(values):
    high = values.astype(BF16)
    rest = values - high.astype(F32)
    mid = rest.astype(BF16)
    low = (rest - mid.astype(F32)).astype(BF16)
    return high, mid, low


def exact_pick(values, onehot):
    high, mid, low = parts(values)
    return dot(high, onehot) + dot(mid, onehot) + dot(low, onehot)


def hidden_pick(q):
    i = iota((128, 1024), 0)
    h = iota((128, 1024), 1)
    return jnp.where(h == (i // 4) * 32 + q * 4 + i % 4, 1.0, 0.0).astype(BF16)


def lane_picks():
    lane = iota((128, 1024), 0)
    i = iota((128, 1024), 1)
    return jnp.where(lane == ((i % 16) // 4) * 32 + (i // 128) * 4 + i % 4, 1.0, 0.0).astype(BF16)


def lane_put(q):
    i = iota((128, 128), 0)
    lane = iota((128, 128), 1)
    return jnp.where(lane == ((i % 16) // 4) * 32 + q * 4 + i % 4, 1.0, 0.0).astype(BF16)


def mish_terms(val):
    u = jnp.exp(jnp.minimum(val, 20.0))
    n = u * (u + 2.0)
    r = 1.0 / (n + 2.0)
    return u, n, r


def kernel(
    count_ref, ids_hbm, scale_hbm, shift_hbm, gain_hbm, bias_hbm, wcode_hbm, wout_hbm, cot_hbm, obias_hbm,
    emb_ref, gcode_ref, gout_ref, ggain_ref, gbias_ref,
    ids_ref, scale_ref, shift_ref, gain_ref, bias_ref, wcode_ref, wout_ref, cot_ref, obias_ref, s_in,
    idf, delta, code, pre, gact, dval, act, wown, wout_own, vec, put, pick_all, mix, nat, own, share, met,
    st_out, st, st2_own, st2, par, tot, p_send, p_recv, a_send, a_recv,
    s_sh, r_sh, s_id, r_id, s_dl, s_df, r_dl, s_st, r_st, s_p, r_p, s_par, r_par, s_st2, r_st2, s_a, r_a, s_tot, r_tot,
):
    z, x, y, c = (lax.axis_index(a) for a in AXES)
    q = y * 2 + c
    zx = z * 4 + x

    z_at = [lax.rem(z + d, 8) for d in range(8)]
    x_at = [lax.rem(x + d, 4) for d in range(4)]
    x_half = [t // 2 for t in x_at]
    x_odd = [lax.rem(t, 2) for t in x_at]
    far = [(z_at[dz], x_at[dx], y, c) for dz, dx in FAR]
    across = [(z_at[dz], x_at[dx], y, 1 - c) for dz, dx in FAR]
    far_zero = [(z_at[dz], x_at[dx], y, 0) for dz, dx in FAR]
    far_hub = [(z_at[dz], x_at[dx], y, 1) for dz, dx in FAR]
    hub = c == 1
    y_at = [lax.rem(y + d, 4) for d in range(4)]
    c_at = [c, 1 - c]
    near = [(z, x, y_at[dy], c_at[dc]) for dy, dc in NEAR]

    loads = [
        pltpu.make_async_copy(src, dst, s_in.at[i])
        for i, (src, dst) in enumerate(
            (
                (ids_hbm, ids_ref),
                (scale_hbm, scale_ref),
                (shift_hbm, shift_ref),
                (wcode_hbm, wcode_ref),
                (cot_hbm, cot_ref),
                (wout_hbm, wout_ref),
                (gain_hbm, gain_ref),
                (bias_hbm, bias_ref),
                (obias_hbm, obias_ref),
            )
        )
    ]
    for load in loads:
        load.start()

    barrier = pltpu.get_barrier_semaphore()

    for device in [d for pair in zip(across, far) for d in pair] + near[1:]:
        pl.semaphore_signal(barrier, inc=1, device_id=device, device_id_type=MESH)

    def send(src, dst, send_sem, recv_sem, device):
        pltpu.make_async_remote_copy(
            src, dst, send_sem, recv_sem, device_id=device, device_id_type=MESH
        ).start()

    def to_near(buf, send_sem, recv_sem):
        for device in near[1:]:
            send(buf.at[q], buf.at[q], send_sem, recv_sem, device)

    def scatter_far(src, dst, send_sem, recv_sem):
        for (dz, dx), device in zip(FAR, far):
            send(src.at[z_at[dz] * 2 + x_half[dx], x_odd[dx]], dst.at[zx], send_sem, recv_sem, device)

    def wait(buf, n, sem):
        part = buf.at[pl.ds(0, n)]
        pltpu.make_async_copy(part, part, sem).wait()

    count = count_ref[0]
    loads[0].wait()
    slot = iota((2, 128), 0) * 128 + iota((2, 128), 1)
    idf[0] = jnp.where(slot < count, ids_ref[...].astype(F32), -1.0)
    for load in loads[1:3]:
        load.wait()
    scale = scale_ref[...].astype(F32)
    high = scale * 256.0
    high = high - ((high * (1.0 / MODULUS) + MAGIC) - MAGIC) * float(MODULUS)
    table = []
    for v in (high, scale, shift_ref[...].astype(F32)):
        coarse = jnp.floor(v * (1.0 / 256.0)) * 256.0
        table += [coarse, v - coarse]
    table = jnp.concatenate(table + [jnp.zeros((10, CODES), F32)], axis=0)
    flag = jnp.where(iota((16, 128), 0) == 6, 1.0, 0.0)
    mix[...] = jnp.concatenate([table, flag], axis=1).astype(BF16)

    def hash_rows(k):
        ident = jnp.concatenate([idf[k, 0:1, :], idf[k, 1:2, :]], axis=1)
        upper = jnp.floor(ident * (1.0 / 256.0))
        lower = ident - upper * 256.0
        alive = jnp.where(ident >= 0.0, 1.0, 0.0)
        row = iota((16, ROWS), 0)
        terms = jnp.where(row < 2, upper, jnp.where(row < 4, lower, jnp.where(row < 6, 1.0, jnp.where(row < 7, alive, 0.0))))
        mixed = dot(terms.astype(BF16), mix[...], TN)
        value = mixed[:, :CODES]
        times = (value * (1.0 / MODULUS) + MAGIC) - MAGIC
        bucket = value - times * float(MODULUS)
        bucket = jnp.where(bucket < 0.0, bucket + float(MODULUS), bucket)
        return bucket * (2.0 / (MODULUS - 1)) - 1.0, mixed[:, CODES:]

    def hash_other(k):
        rows, alive = hash_rows(k)
        rows = rows.astype(BF16)
        code[k * ROWS : k * ROWS + ROWS, :] = rows
        pre[k * ROWS : k * ROWS + ROWS, :] = dot(rows, wown[...]) * alive

    rows, alive = hash_rows(0)
    rows = (rows * jnp.concatenate([alive] * 4, axis=1)).astype(BF16)
    code[0:ROWS, :] = rows
    pick_all[...] = lane_picks()
    own_z = iota((8, 128), 0) == iota((8, 128), 1) // 16
    loads[3].wait()
    rows_of = []
    for k in range(GROUP):
        hidden = dot(rows, wcode_ref[:, k * 128 : k * 128 + 128])
        own[:, k * 128 : k * 128 + 128] = hidden
        rows_of.append((jnp.sum(hidden, axis=0, keepdims=True), jnp.sum(hidden * hidden, axis=0, keepdims=True)))
    by_z = jnp.concatenate([r[v] for v in range(2) for r in rows_of], axis=0)
    by_unit = dot(jnp.concatenate(parts(by_z), axis=0), pick_all[...])
    by_unit = by_unit[0:16] + by_unit[16:32] + by_unit[32:48]
    for k in range(GROUP):
        unit = by_unit[:, k * 128 : k * 128 + 128]
        share[k // 2, k % 2] = jnp.concatenate(
            [jnp.sum(jnp.where(own_z, unit[8 * v : 8 * v + 8], 0.0), axis=0, keepdims=True) for v in range(2)], axis=0
        )

    pl.semaphore_wait(barrier, 2 * (PEERS - 1) + GROUP - 1)
    for dy in (2, 1, 3):
        send(share.at[y_at[dy]], met.at[(4 - dy) * 2 + 1 - c], s_sh, r_sh, (z, x, y_at[dy], 1))

    @pl.when(hub)
    def _():
        met[0] = share[y]

    @pl.when(c == 0)
    def _():
        send(share.at[y], met.at[1], s_sh, r_sh, (z, x, y, 1))

    for k in range(1, GROUP):
        send(idf.at[0], idf.at[BACK[k]], s_id, r_id.at[BACK[k]], near[k])

    loads[4].wait()
    live = iota((ROWS, 128), 0) < count
    delta[0] = jnp.where(live, cot_ref[...].astype(F32) * (1.0 / 128.0), 0.0).astype(BF16)
    for k in (2, 3, 6, 1):
        send(delta.at[0], delta.at[BACK[k]], s_dl, r_dl.at[BACK[k]], near[k])

    for load in loads[5:]:
        load.wait()
    pick = hidden_pick(q)
    wown[...] = dot(wcode_ref[...], pick, NT).astype(BF16)

    pre[0:ROWS, :] = dot(code[0:ROWS, :], wown[...])
    wout_own[...] = dot(pick, wout_ref[...]).astype(BF16)
    small = pick_all[:, pl.ds(pl.multiple_of(q * 128, 128), 128)]
    vec[0:1] = jnp.sum(jnp.where(own_z, exact_pick(gain_ref[...], small), 0.0), axis=0, keepdims=True)
    vec[1:2] = jnp.sum(jnp.where(own_z, exact_pick(bias_ref[...], small), 0.0), axis=0, keepdims=True)
    for b in range(GROUP):
        put[b * 128 : b * 128 + 128, :] = lane_put(b)
    pltpu.make_async_copy(idf.at[1], idf.at[1], r_id.at[1]).wait()
    hash_other(1)

    @pl.when(hub)
    def _():
        wait(met, GROUP - 1, r_sh)
        both = jnp.sum(met[...], axis=0)
        st_out[...] = both
        st[zx] = both[1]
        for zero, one in zip(far_zero, far_hub):
            send(st_out.at[0], st.at[zx], s_st, r_st, zero)
            send(st_out.at[1], st.at[zx], s_st, r_st, one)
        send(st_out.at[0], st.at[zx], s_st, r_st, (z, x, y, 0))

    def arrived(k):
        pltpu.make_async_copy(delta.at[k], delta.at[k], r_dl.at[k]).wait()

    for batch, passed in (((2, 3), ()), ((4, 5), (2, 3)), ((6, 7), (6,))):
        for k in batch:
            pltpu.make_async_copy(idf.at[k], idf.at[k], r_id.at[k]).wait()
        for k in batch:
            hash_other(k)
        for k in passed:
            arrived(k)
            send(delta.at[k], delta.at[ACROSS[k]], s_df, r_dl.at[ACROSS[k]], near[1])

    def pack(buf, full, last):
        for parity in range(2):
            lo = parity * 4
            tiles = full.reshape(16, 8, CODES)[:, lo : lo + 4, :]
            for b in range(4):
                buf[:, parity, b] = tiles[:, :, b * 128 : b * 128 + 128].astype(BF16)
            buf[:, parity, 4] = last[:, lo : lo + 4, :].astype(BF16)

    alive = jnp.concatenate([jnp.where(idf[b, h : h + 1, :] >= 0.0, 1.0, 0.0) for b in range(8) for h in range(2)], axis=1)
    code_sum = dot(jnp.broadcast_to(alive, (8, GROUP * ROWS)).astype(BF16), code[...])[0:1]
    s_rows = jnp.concatenate([code_sum[:, 128 * i : 128 * i + 128] for i in range(4)] * 2, axis=0)
    pack(p_send, dot(pre[...].astype(BF16), code[...], TN), jnp.broadcast_to(s_rows[None], (16, 8, 128)))
    p_recv[zx] = p_send[zx // 2, lax.rem(zx, 2)]
    scatter_far(p_send, p_recv, s_p, r_p)

    for k in range(GROUP):
        if k in (1, 4, 5, 7):
            arrived(k)
        gact[k * ROWS : k * ROWS + ROWS, :] = dot(delta[k], wout_own[...], NT)

    def in_order(row):
        blocks = [jnp.concatenate([jnp.where(own_z, row(b, v), 0.0) for b in range(GROUP)], axis=1) for v in range(2)]
        out = dot(jnp.concatenate(parts(jnp.concatenate(blocks, axis=0)), axis=0), put[...])
        return out[0:16] + out[16:32] + out[32:48]

    @pl.when(hub)
    def _():
        wait(st, PEERS - 1, r_st)

    @pl.when(c == 0)
    def _():
        wait(st, PEERS, r_st)

    moments = jnp.sum(st[...], axis=0) * (1.0 / TOTAL)
    mean = moments[0:1]
    inv_std = lax.rsqrt(moments[1:2] - mean * mean + EPSILON)
    gain = vec[0:1]
    bias = vec[1:2]
    par[q] = jnp.concatenate([mean, inv_std], axis=0)
    to_near(par, s_par, r_par)

    slope_in = inv_std * gain

    def second(b, carry):
        sum_gain, sum_bias = carry
        at = pl.multiple_of(b * ROWS, ROWS)
        centred = pre[pl.ds(at, ROWS), :] - mean
        val = centred * slope_in + bias
        u, n, r = mish_terms(val)
        ratio = val * r
        act[b] = (n * ratio).astype(BF16)
        slope = r * (n + 4.0 * ((n - u) * ratio))
        d = gact[pl.ds(at, ROWS), :] * slope
        dval[pl.ds(at, ROWS), :] = d.astype(BF16)
        return (
            sum_gain + jnp.sum(d * centred, axis=0, keepdims=True),
            sum_bias + jnp.sum(d, axis=0, keepdims=True),
        )

    zero = jnp.zeros((1, 128), F32)
    sums = lax.fori_loop(0, GROUP, second, (zero, zero))
    mine2 = jnp.concatenate([sums[0] * inv_std, sums[1]], axis=0)
    st2_own[...] = mine2
    for one in far_hub:
        send(st2_own, st2.at[c * PEERS + zx], s_st2, r_st2, one)

    @pl.when(hub)
    def _():
        st2[PEERS + zx] = mine2

    @pl.when(c == 0)
    def _():
        send(st2_own, st2.at[zx], s_st2, r_st2, (z, x, y, 1))


    a_full = dot(dval[...], code[...], TN)
    o_full = dot(act[...].reshape(GROUP * ROWS, 128), delta[...].reshape(GROUP * ROWS, 128), TN)
    pack(a_send, a_full, o_full.reshape(16, 8, 128))
    a_recv[zx] = a_send[zx // 2, lax.rem(zx, 2)]
    scatter_far(a_send, a_recv, s_a, r_a)

    wait(par, GROUP - 1, r_par)
    ordered = in_order(lambda b, v: par[b, v : v + 1, :])
    nat[0] = ordered[0:8]
    nat[1] = ordered[8:16] * gain_ref[...]

    acc = jnp.zeros((ROWS, 128), F32)
    for k in range(GROUP):
        hidden = own[:, k * 128 : k * 128 + 128]
        val = (hidden - nat[0, k : k + 1, :]) * nat[1, k : k + 1, :] + bias_ref[k : k + 1, :]
        _, n, r = mish_terms(val)
        acc = acc + dot((n * (val * r)).astype(BF16), wout_ref[k * 128 : k * 128 + 128, :])
    live = iota((ROWS, 128), 0) < count
    emb_ref[...] = jnp.where(live, acc + obias_ref[...], 0.0).astype(BF16)

    @pl.when(hub)
    def _():
        wait(st2, 2 * PEERS - 1, r_st2)
        for v in range(2):
            tot[y, v] = jnp.sum(st2[v * PEERS : v * PEERS + PEERS], axis=0)
        for dy in (2, 1, 3):
            for core in (0, 1):
                send(tot.at[y], tot.at[y], s_tot, r_tot, (z, x, y_at[dy], core))
        send(tot.at[y], tot.at[y], s_tot, r_tot, (z, x, y, 0))

    wait(p_recv, PEERS - 1, r_p)
    p_sum = jnp.sum(p_recv[...].astype(F32), axis=0)
    wait(a_recv, PEERS - 1, r_a)
    a_sum = jnp.sum(a_recv[...].astype(F32), axis=0)
    gout_ref[...] = a_sum[4]

    @pl.when(hub)
    def _():
        wait(tot, 3, r_tot)

    @pl.when(c == 0)
    def _():
        wait(tot, 4, r_tot)

    ordered = in_order(lambda b, v: tot[b // 2, b % 2, v : v + 1, :])
    ggain_ref[...] = ordered[0:8]
    gbias_ref[...] = ordered[8:16]

    sums = tot[y, c]
    k1 = inv_std * gain
    k3 = k1 * inv_std * sums[0:1] * (1.0 / TOTAL)
    k2 = k1 * sums[1:2] * (1.0 / TOTAL) - k3 * mean
    mine = iota((4, 128), 1) == zx * 4 + iota((4, 128), 0)

    def column(v):
        return jnp.sum(jnp.where(mine, v, 0.0), axis=1, keepdims=True)

    k1, k2, k3 = column(k1), column(k2), column(k3)
    gcode_ref[...] = jnp.concatenate(
        [k1 * a_sum[b] - k2 * p_sum[4, b : b + 1, :] - k3 * p_sum[b] for b in range(4)], axis=1
    )

    @pl.when(hub)
    def _():
        wait(met, 3, s_sh)
        wait(st2, 2 * PEERS - 1, s_st)
        wait(st2, PEERS - 1, s_st2)
        wait(met, GROUP - 1, s_tot)

    @pl.when(c == 0)
    def _():
        wait(met, 4, s_sh)
        wait(st2, PEERS, s_st2)

    wait(idf, GROUP - 1, s_id)
    wait(delta, 4, s_dl)
    wait(delta, 3, s_df)
    wait(p_recv, PEERS - 1, s_p)
    wait(par, GROUP - 1, s_par)
    wait(a_recv, PEERS - 1, s_a)


def store_kernel(*refs):
    srcs, dsts, sem = refs[:5], refs[5:10], refs[10]
    copies = [pltpu.make_async_copy(a, b, sem.at[i]) for i, (a, b) in enumerate(zip(srcs, dsts))]
    for copy in copies:
        copy.start()
    for copy in copies:
        copy.wait()


def per_device(ids, counts, hash_scale, hash_shift, w_code, norm_gain, norm_bias, w_out, out_bias, cotangent):
    vmem = pl.BlockSpec(memory_space=pltpu.VMEM)
    hbm = pl.BlockSpec(memory_space=pltpu.HBM)
    dma = pltpu.SemaphoreType.DMA
    wide = GROUP * ROWS
    shapes = (
        jax.ShapeDtypeStruct((ROWS, 128), BF16),
        jax.ShapeDtypeStruct((4, CODES), F32),
        jax.ShapeDtypeStruct((4, 128), F32),
        jax.ShapeDtypeStruct((8, 128), F32),
        jax.ShapeDtypeStruct((8, 128), F32),
    )
    results = pl.pallas_call(
        kernel,
        out_shape=shapes,
        in_specs=[pl.BlockSpec(memory_space=pltpu.SMEM)] + [hbm] * 9,
        out_specs=(vmem,) * 5,
        scratch_shapes=[
            pltpu.VMEM((2, 128), jnp.int32),
            pltpu.VMEM((1, CODES), jnp.int32),
            pltpu.VMEM((1, CODES), jnp.int32),
            pltpu.VMEM((8, 128), F32),
            pltpu.VMEM((8, 128), F32),
            pltpu.VMEM((CODES, 1024), BF16),
            pltpu.VMEM((1024, 128), BF16),
            pltpu.VMEM((ROWS, 128), BF16),
            pltpu.VMEM((1, 128), F32),
            dma((9,)),
            pltpu.VMEM((GROUP, 2, 128), F32),
            pltpu.VMEM((GROUP, ROWS, 128), BF16),
            pltpu.VMEM((wide, CODES), BF16),
            pltpu.VMEM((wide, 128), F32),
            pltpu.VMEM((wide, 128), F32),
            pltpu.VMEM((wide, 128), BF16),
            pltpu.VMEM((GROUP, ROWS, 128), BF16),
            pltpu.VMEM((CODES, 128), BF16),
            pltpu.VMEM((128, 128), BF16),
            pltpu.VMEM((8, 128), F32),
            pltpu.VMEM((1024, 128), BF16),
            pltpu.VMEM((128, 1024), BF16),
            pltpu.VMEM((16, CODES + 128), BF16),
            pltpu.VMEM((2, 8, 128), F32),
            pltpu.VMEM((ROWS, 1024), F32),
            pltpu.VMEM((4, 2, 2, 128), F32),
            pltpu.VMEM((GROUP, 2, 2, 128), F32),
            pltpu.VMEM((2, 2, 128), F32),
            pltpu.VMEM((PEERS, 2, 128), F32),
            pltpu.VMEM((2, 128), F32),
            pltpu.VMEM((2 * PEERS, 2, 128), F32),
            pltpu.VMEM((GROUP, 2, 128), F32),
            pltpu.VMEM((4, 2, 2, 128), F32),
            pltpu.VMEM((16, 2, 5, 4, 128), BF16),
            pltpu.VMEM((PEERS, 5, 4, 128), BF16),
            pltpu.VMEM((16, 2, 5, 4, 128), BF16),
            pltpu.VMEM((PEERS, 5, 4, 128), BF16),
        ]
        + [dma, dma, dma, dma((GROUP,)), dma, dma, dma((GROUP,))]
        + [dma] * 12,
        compiler_params=pltpu.CompilerParams(
            collective_id=0, has_side_effects=True, vmem_limit_bytes=48 << 20
        ),
    )(
        counts,
        *(
            pltpu.with_memory_space_constraint(array, pltpu.HBM)
            for array in (
                ids.reshape(2, 128),
                hash_scale.reshape(1, CODES),
                hash_shift.reshape(1, CODES),
                norm_gain.reshape(8, 128),
                norm_bias.reshape(8, 128),
                w_code,
                w_out,
                cotangent,
                out_bias.reshape(1, 128),
            )
        ),
    )
    emb, gcode, gout, ggain, gbias = pl.pallas_call(
        store_kernel,
        out_shape=shapes,
        in_specs=[vmem] * 5,
        out_specs=(hbm,) * 5,
        scratch_shapes=[dma((5,))],
        compiler_params=pltpu.CompilerParams(vmem_limit_bytes=4 << 20),
    )(*results)
    return emb, gcode, gout, ggain.reshape(1024), gbias.reshape(1024)


def solution(mesh):
    finer = Mesh(mesh.devices.reshape(8, 4, 4, 2), AXES)
    return jax.shard_map(
        per_device,
        mesh=finer,
        in_specs=(P(AXES), P(AXES), P(), P(), P(), P(), P(), P(), P(), P(AXES, None)),
        out_specs=(P(AXES, None), P(AXES, None), P(AXES, None), P(), P()),
        check_vma=False,
    )
```

```python
import functools

import jax
import jax.numpy as jnp
from jax import lax
from jax.experimental import pallas as pl
from jax.experimental.pallas import tpu as pltpu
from jax.sharding import Mesh
from jax.sharding import PartitionSpec as P

AXES = ("z", "x", "y", "c")
MESH = pl.DeviceIdType.MESH
F32 = jnp.float32
BF16 = jnp.bfloat16
MODULUS = 65521
EPSILON = 1e-05
MAGIC = 12582912.0
TOTAL = 16384.0
ROWS = 256
CODES = 512
GROUP = 8
PEERS = 32
FAR = sorted(
    ((dz, dx) for dz in range(8) for dx in range(4) if dz or dx),
    key=lambda o: (-min(o[0], 8 - o[0]) - min(o[1], 4 - o[1]), o),
)
NEAR = [(0, 0), (0, 1), (1, 0), (3, 0), (1, 1), (3, 1), (2, 0), (2, 1)]
ACROSS = {k: NEAR.index((NEAR[k][0], 1)) for k in (2, 3, 6)}
BACK = [NEAR.index(((4 - dy) % 4, dc)) for dy, dc in NEAR]

NN = (((1,), (0,)), ((), ()))
NT = (((1,), (1,)), ((), ()))
TN = (((0,), (0,)), ((), ()))


def dot(a, b, dims=NN):
    return lax.dot_general(a, b, dims, preferred_element_type=F32)


def iota(shape, dim):
    return lax.broadcasted_iota(jnp.int32, shape, dim)


def parts(values):
    high = values.astype(BF16)
    rest = values - high.astype(F32)
    mid = rest.astype(BF16)
    low = (rest - mid.astype(F32)).astype(BF16)
    return high, mid, low


def exact_pick(values, onehot):
    high, mid, low = parts(values)
    return dot(high, onehot) + dot(mid, onehot) + dot(low, onehot)


def hidden_pick(q):
    i = iota((128, 1024), 0)
    h = iota((128, 1024), 1)
    return jnp.where(h == (i // 4) * 32 + q * 4 + i % 4, 1.0, 0.0).astype(BF16)


def lane_picks():
    lane = iota((128, 1024), 0)
    i = iota((128, 1024), 1)
    return jnp.where(lane == ((i % 16) // 4) * 32 + (i // 128) * 4 + i % 4, 1.0, 0.0).astype(BF16)


def lane_put(q):
    i = iota((128, 128), 0)
    lane = iota((128, 128), 1)
    return jnp.where(lane == ((i % 16) // 4) * 32 + q * 4 + i % 4, 1.0, 0.0).astype(BF16)


def mish_terms(val):
    u = jnp.exp(jnp.minimum(val, 20.0))
    n = u * (u + 2.0)
    r = 1.0 / (n + 2.0)
    return u, n, r


def kernel(
    count_ref, ids_hbm, scale_hbm, shift_hbm, gain_hbm, bias_hbm, wcode_hbm, wout_hbm, cot_hbm, obias_hbm,
    emb_ref, gcode_ref, gout_ref, ggain_ref, gbias_ref,
    ids_ref, scale_ref, shift_ref, gain_ref, bias_ref, wcode_ref, wout_ref, cot_ref, obias_ref, s_in,
    idf, delta, code, pre, gact, dval, act, wown, wout_own, vec, put, pick_all, mix, nat, own, share, met,
    st_out, st, st2_own, st2, par, tot, p_send, p_recv, a_send, a_recv,
    s_sh, r_sh, s_id, r_id, s_dl, s_df, r_dl, s_st, r_st, s_p, r_p, s_par, r_par, s_st2, r_st2, s_a, r_a, s_tot, r_tot,
):
    z, x, y, c = (lax.axis_index(a) for a in AXES)
    q = y * 2 + c
    zx = z * 4 + x

    z_at = [lax.rem(z + d, 8) for d in range(8)]
    x_at = [lax.rem(x + d, 4) for d in range(4)]
    x_half = [t // 2 for t in x_at]
    x_odd = [lax.rem(t, 2) for t in x_at]
    far = [(z_at[dz], x_at[dx], y, c) for dz, dx in FAR]
    across = [(z_at[dz], x_at[dx], y, 1 - c) for dz, dx in FAR]
    far_zero = [(z_at[dz], x_at[dx], y, 0) for dz, dx in FAR]
    far_hub = [(z_at[dz], x_at[dx], y, 1) for dz, dx in FAR]
    hub = c == 1
    y_at = [lax.rem(y + d, 4) for d in range(4)]
    c_at = [c, 1 - c]
    near = [(z, x, y_at[dy], c_at[dc]) for dy, dc in NEAR]

    loads = [
        pltpu.make_async_copy(src, dst, s_in.at[i])
        for i, (src, dst) in enumerate(
            (
                (ids_hbm, ids_ref),
                (scale_hbm, scale_ref),
                (shift_hbm, shift_ref),
                (wcode_hbm, wcode_ref),
                (cot_hbm, cot_ref),
                (wout_hbm, wout_ref),
                (gain_hbm, gain_ref),
                (bias_hbm, bias_ref),
                (obias_hbm, obias_ref),
            )
        )
    ]
    for load in loads:
        load.start()

    barrier = pltpu.get_barrier_semaphore()

    for device in [d for pair in zip(across, far) for d in pair] + near[1:]:
        pl.semaphore_signal(barrier, inc=1, device_id=device, device_id_type=MESH)

    def send(src, dst, send_sem, recv_sem, device):
        pltpu.make_async_remote_copy(
            src, dst, send_sem, recv_sem, device_id=device, device_id_type=MESH
        ).start()

    def to_near(buf, send_sem, recv_sem):
        for device in near[1:]:
            send(buf.at[q], buf.at[q], send_sem, recv_sem, device)

    def scatter_far(src, dst, send_sem, recv_sem):
        for (dz, dx), device in zip(FAR, far):
            send(src.at[z_at[dz] * 2 + x_half[dx], x_odd[dx]], dst.at[zx], send_sem, recv_sem, device)

    def wait(buf, n, sem):
        part = buf.at[pl.ds(0, n)]
        pltpu.make_async_copy(part, part, sem).wait()

    count = count_ref[0]
    loads[0].wait()
    slot = iota((2, 128), 0) * 128 + iota((2, 128), 1)
    idf[0] = jnp.where(slot < count, ids_ref[...].astype(F32), -1.0)
    for load in loads[1:3]:
        load.wait()
    scale = scale_ref[...].astype(F32)
    high = scale * 256.0
    high = high - ((high * (1.0 / MODULUS) + MAGIC) - MAGIC) * float(MODULUS)
    table = []
    for v in (high, scale, shift_ref[...].astype(F32)):
        coarse = jnp.floor(v * (1.0 / 256.0)) * 256.0
        table += [coarse, v - coarse]
    table = jnp.concatenate(table + [jnp.zeros((10, CODES), F32)], axis=0)
    flag = jnp.where(iota((16, 128), 0) == 6, 1.0, 0.0)
    mix[...] = jnp.concatenate([table, flag], axis=1).astype(BF16)

    def hash_rows(k):
        ident = jnp.concatenate([idf[k, 0:1, :], idf[k, 1:2, :]], axis=1)
        upper = jnp.floor(ident * (1.0 / 256.0))
        lower = ident - upper * 256.0
        alive = jnp.where(ident >= 0.0, 1.0, 0.0)
        row = iota((16, ROWS), 0)
        terms = jnp.where(row < 2, upper, jnp.where(row < 4, lower, jnp.where(row < 6, 1.0, jnp.where(row < 7, alive, 0.0))))
        mixed = dot(terms.astype(BF16), mix[...], TN)
        value = mixed[:, :CODES]
        times = (value * (1.0 / MODULUS) + MAGIC) - MAGIC
        bucket = value - times * float(MODULUS)
        bucket = jnp.where(bucket < 0.0, bucket + float(MODULUS), bucket)
        return bucket * (2.0 / (MODULUS - 1)) - 1.0, mixed[:, CODES:]

    def hash_other(k):
        rows, alive = hash_rows(k)
        rows = rows.astype(BF16)
        code[k * ROWS : k * ROWS + ROWS, :] = rows
        pre[k * ROWS : k * ROWS + ROWS, :] = dot(rows, wown[...]) * alive

    rows, alive = hash_rows(0)
    rows = (rows * jnp.concatenate([alive] * 4, axis=1)).astype(BF16)
    code[0:ROWS, :] = rows
    pick_all[...] = lane_picks()
    own_z = iota((8, 128), 0) == iota((8, 128), 1) // 16
    loads[3].wait()
    rows_of = []
    for k in range(GROUP):
        hidden = dot(rows, wcode_ref[:, k * 128 : k * 128 + 128])
        own[:, k * 128 : k * 128 + 128] = hidden
        rows_of.append((jnp.sum(hidden, axis=0, keepdims=True), jnp.sum(hidden * hidden, axis=0, keepdims=True)))
    by_z = jnp.concatenate([r[v] for v in range(2) for r in rows_of], axis=0)
    by_unit = dot(jnp.concatenate(parts(by_z), axis=0), pick_all[...])
    by_unit = by_unit[0:16] + by_unit[16:32] + by_unit[32:48]
    for k in range(GROUP):
        unit = by_unit[:, k * 128 : k * 128 + 128]
        share[k // 2, k % 2] = jnp.concatenate(
            [jnp.sum(jnp.where(own_z, unit[8 * v : 8 * v + 8], 0.0), axis=0, keepdims=True) for v in range(2)], axis=0
        )

    pl.semaphore_wait(barrier, 2 * (PEERS - 1) + GROUP - 1)
    for dy in (2, 1, 3):
        send(share.at[y_at[dy]], met.at[(4 - dy) * 2 + 1 - c], s_sh, r_sh, (z, x, y_at[dy], 1))

    @pl.when(hub)
    def _():
        met[0] = share[y]

    @pl.when(c == 0)
    def _():
        send(share.at[y], met.at[1], s_sh, r_sh, (z, x, y, 1))

    for k in range(1, GROUP):
        send(idf.at[0], idf.at[BACK[k]], s_id, r_id.at[BACK[k]], near[k])

    loads[4].wait()
    live = iota((ROWS, 128), 0) < count
    delta[0] = jnp.where(live, cot_ref[...].astype(F32) * (1.0 / 128.0), 0.0).astype(BF16)
    for k in (2, 3, 6, 1):
        send(delta.at[0], delta.at[BACK[k]], s_dl, r_dl.at[BACK[k]], near[k])

    for load in loads[5:]:
        load.wait()
    pick = hidden_pick(q)
    wown[...] = dot(wcode_ref[...], pick, NT).astype(BF16)

    pre[0:ROWS, :] = dot(code[0:ROWS, :], wown[...])
    wout_own[...] = dot(pick, wout_ref[...]).astype(BF16)
    small = pick_all[:, pl.ds(pl.multiple_of(q * 128, 128), 128)]
    vec[0:1] = jnp.sum(jnp.where(own_z, exact_pick(gain_ref[...], small), 0.0), axis=0, keepdims=True)
    vec[1:2] = jnp.sum(jnp.where(own_z, exact_pick(bias_ref[...], small), 0.0), axis=0, keepdims=True)
    for b in range(GROUP):
        put[b * 128 : b * 128 + 128, :] = lane_put(b)
    pltpu.make_async_copy(idf.at[1], idf.at[1], r_id.at[1]).wait()
    hash_other(1)

    @pl.when(hub)
    def _():
        wait(met, GROUP - 1, r_sh)
        both = jnp.sum(met[...], axis=0)
        st_out[...] = both
        st[zx] = both[1]
        for zero, one in zip(far_zero, far_hub):
            send(st_out.at[0], st.at[zx], s_st, r_st, zero)
            send(st_out.at[1], st.at[zx], s_st, r_st, one)
        send(st_out.at[0], st.at[zx], s_st, r_st, (z, x, y, 0))

    def arrived(k):
        pltpu.make_async_copy(delta.at[k], delta.at[k], r_dl.at[k]).wait()

    for batch, passed in (((2, 3, 4, 5, 6, 7), (2, 3, 6)),):
        for k in batch:
            pltpu.make_async_copy(idf.at[k], idf.at[k], r_id.at[k]).wait()
        for k in batch:
            hash_other(k)
        for k in passed:
            arrived(k)
            send(delta.at[k], delta.at[ACROSS[k]], s_df, r_dl.at[ACROSS[k]], near[1])

    def pack(buf, full, last):
        for parity in range(2):
            lo = parity * 4
            tiles = full.reshape(16, 8, CODES)[:, lo : lo + 4, :]
            for b in range(4):
                buf[:, parity, b] = tiles[:, :, b * 128 : b * 128 + 128].astype(BF16)
            buf[:, parity, 4] = last[:, lo : lo + 4, :].astype(BF16)

    alive = jnp.concatenate([jnp.where(idf[b, h : h + 1, :] >= 0.0, 1.0, 0.0) for b in range(8) for h in range(2)], axis=1)
    code_sum = dot(jnp.broadcast_to(alive, (8, GROUP * ROWS)).astype(BF16), code[...])[0:1]
    s_rows = jnp.concatenate([code_sum[:, 128 * i : 128 * i + 128] for i in range(4)] * 2, axis=0)
    pack(p_send, dot(pre[...].astype(BF16), code[...], TN), jnp.broadcast_to(s_rows[None], (16, 8, 128)))
    p_recv[zx] = p_send[zx // 2, lax.rem(zx, 2)]
    scatter_far(p_send, p_recv, s_p, r_p)

    for k in range(GROUP):
        if k in (1, 4, 5, 7):
            arrived(k)
        gact[k * ROWS : k * ROWS + ROWS, :] = dot(delta[k], wout_own[...], NT)

    def in_order(row):
        blocks = [jnp.concatenate([jnp.where(own_z, row(b, v), 0.0) for b in range(GROUP)], axis=1) for v in range(2)]
        out = dot(jnp.concatenate(parts(jnp.concatenate(blocks, axis=0)), axis=0), put[...])
        return out[0:16] + out[16:32] + out[32:48]

    @pl.when(hub)
    def _():
        wait(st, PEERS - 1, r_st)

    @pl.when(c == 0)
    def _():
        wait(st, PEERS, r_st)

    moments = jnp.sum(st[...], axis=0) * (1.0 / TOTAL)
    mean = moments[0:1]
    inv_std = lax.rsqrt(moments[1:2] - mean * mean + EPSILON)
    gain = vec[0:1]
    bias = vec[1:2]
    par[q] = jnp.concatenate([mean, inv_std], axis=0)
    to_near(par, s_par, r_par)

    slope_in = inv_std * gain

    def second(b, carry):
        sum_gain, sum_bias = carry
        at = pl.multiple_of(b * ROWS, ROWS)
        centred = pre[pl.ds(at, ROWS), :] - mean
        val = centred * slope_in + bias
        u, n, r = mish_terms(val)
        ratio = val * r
        act[b] = (n * ratio).astype(BF16)
        slope = r * (n + 4.0 * ((n - u) * ratio))
        d = gact[pl.ds(at, ROWS), :] * slope
        dval[pl.ds(at, ROWS), :] = d.astype(BF16)
        return (
            sum_gain + jnp.sum(d * centred, axis=0, keepdims=True),
            sum_bias + jnp.sum(d, axis=0, keepdims=True),
        )

    zero = jnp.zeros((1, 128), F32)
    sums = lax.fori_loop(0, GROUP, second, (zero, zero))
    mine2 = jnp.concatenate([sums[0] * inv_std, sums[1]], axis=0)
    st2_own[...] = mine2
    for one in far_hub:
        send(st2_own, st2.at[c * PEERS + zx], s_st2, r_st2, one)

    @pl.when(hub)
    def _():
        st2[PEERS + zx] = mine2

    @pl.when(c == 0)
    def _():
        send(st2_own, st2.at[zx], s_st2, r_st2, (z, x, y, 1))


    a_full = dot(dval[...], code[...], TN)
    o_full = dot(act[...].reshape(GROUP * ROWS, 128), delta[...].reshape(GROUP * ROWS, 128), TN)
    pack(a_send, a_full, o_full.reshape(16, 8, 128))
    a_recv[zx] = a_send[zx // 2, lax.rem(zx, 2)]
    scatter_far(a_send, a_recv, s_a, r_a)

    wait(par, GROUP - 1, r_par)
    ordered = in_order(lambda b, v: par[b, v : v + 1, :])
    nat[0] = ordered[0:8]
    nat[1] = ordered[8:16] * gain_ref[...]

    acc = jnp.zeros((ROWS, 128), F32)
    for k in range(GROUP):
        hidden = own[:, k * 128 : k * 128 + 128]
        val = (hidden - nat[0, k : k + 1, :]) * nat[1, k : k + 1, :] + bias_ref[k : k + 1, :]
        _, n, r = mish_terms(val)
        acc = acc + dot((n * (val * r)).astype(BF16), wout_ref[k * 128 : k * 128 + 128, :])
    live = iota((ROWS, 128), 0) < count
    emb_ref[...] = jnp.where(live, acc + obias_ref[...], 0.0).astype(BF16)

    @pl.when(hub)
    def _():
        wait(st2, 2 * PEERS - 1, r_st2)
        for v in range(2):
            tot[y, v] = jnp.sum(st2[v * PEERS : v * PEERS + PEERS], axis=0)
        for dy in (2, 1, 3):
            for core in (0, 1):
                send(tot.at[y], tot.at[y], s_tot, r_tot, (z, x, y_at[dy], core))
        send(tot.at[y], tot.at[y], s_tot, r_tot, (z, x, y, 0))

    wait(p_recv, PEERS - 1, r_p)
    p_sum = jnp.sum(p_recv[...].astype(F32), axis=0)
    wait(a_recv, PEERS - 1, r_a)
    a_sum = jnp.sum(a_recv[...].astype(F32), axis=0)
    gout_ref[...] = a_sum[4]

    @pl.when(hub)
    def _():
        wait(tot, 3, r_tot)

    @pl.when(c == 0)
    def _():
        wait(tot, 4, r_tot)

    ordered = in_order(lambda b, v: tot[b // 2, b % 2, v : v + 1, :])
    ggain_ref[...] = ordered[0:8]
    gbias_ref[...] = ordered[8:16]

    sums = tot[y, c]
    k1 = inv_std * gain
    k3 = k1 * inv_std * sums[0:1] * (1.0 / TOTAL)
    k2 = k1 * sums[1:2] * (1.0 / TOTAL) - k3 * mean
    mine = iota((4, 128), 1) == zx * 4 + iota((4, 128), 0)

    def column(v):
        return jnp.sum(jnp.where(mine, v, 0.0), axis=1, keepdims=True)

    k1, k2, k3 = column(k1), column(k2), column(k3)
    gcode_ref[...] = jnp.concatenate(
        [k1 * a_sum[b] - k2 * p_sum[4, b : b + 1, :] - k3 * p_sum[b] for b in range(4)], axis=1
    )

    @pl.when(hub)
    def _():
        wait(met, 3, s_sh)
        wait(st2, 2 * PEERS - 1, s_st)
        wait(st2, PEERS - 1, s_st2)
        wait(met, GROUP - 1, s_tot)

    @pl.when(c == 0)
    def _():
        wait(met, 4, s_sh)
        wait(st2, PEERS, s_st2)

    wait(idf, GROUP - 1, s_id)
    wait(delta, 4, s_dl)
    wait(delta, 3, s_df)
    wait(p_recv, PEERS - 1, s_p)
    wait(par, GROUP - 1, s_par)
    wait(a_recv, PEERS - 1, s_a)


def store_kernel(*refs):
    srcs, dsts, sem = refs[:5], refs[5:10], refs[10]
    copies = [pltpu.make_async_copy(a, b, sem.at[i]) for i, (a, b) in enumerate(zip(srcs, dsts))]
    for copy in copies:
        copy.start()
    for copy in copies:
        copy.wait()


def per_device(ids, counts, hash_scale, hash_shift, w_code, norm_gain, norm_bias, w_out, out_bias, cotangent):
    vmem = pl.BlockSpec(memory_space=pltpu.VMEM)
    hbm = pl.BlockSpec(memory_space=pltpu.HBM)
    dma = pltpu.SemaphoreType.DMA
    wide = GROUP * ROWS
    shapes = (
        jax.ShapeDtypeStruct((ROWS, 128), BF16),
        jax.ShapeDtypeStruct((4, CODES), F32),
        jax.ShapeDtypeStruct((4, 128), F32),
        jax.ShapeDtypeStruct((8, 128), F32),
        jax.ShapeDtypeStruct((8, 128), F32),
    )
    results = pl.pallas_call(
        kernel,
        out_shape=shapes,
        in_specs=[pl.BlockSpec(memory_space=pltpu.SMEM)] + [hbm] * 9,
        out_specs=(vmem,) * 5,
        scratch_shapes=[
            pltpu.VMEM((2, 128), jnp.int32),
            pltpu.VMEM((1, CODES), jnp.int32),
            pltpu.VMEM((1, CODES), jnp.int32),
            pltpu.VMEM((8, 128), F32),
            pltpu.VMEM((8, 128), F32),
            pltpu.VMEM((CODES, 1024), BF16),
            pltpu.VMEM((1024, 128), BF16),
            pltpu.VMEM((ROWS, 128), BF16),
            pltpu.VMEM((1, 128), F32),
            dma((9,)),
            pltpu.VMEM((GROUP, 2, 128), F32),
            pltpu.VMEM((GROUP, ROWS, 128), BF16),
            pltpu.VMEM((wide, CODES), BF16),
            pltpu.VMEM((wide, 128), F32),
            pltpu.VMEM((wide, 128), F32),
            pltpu.VMEM((wide, 128), BF16),
            pltpu.VMEM((GROUP, ROWS, 128), BF16),
            pltpu.VMEM((CODES, 128), BF16),
            pltpu.VMEM((128, 128), BF16),
            pltpu.VMEM((8, 128), F32),
            pltpu.VMEM((1024, 128), BF16),
            pltpu.VMEM((128, 1024), BF16),
            pltpu.VMEM((16, CODES + 128), BF16),
            pltpu.VMEM((2, 8, 128), F32),
            pltpu.VMEM((ROWS, 1024), F32),
            pltpu.VMEM((4, 2, 2, 128), F32),
            pltpu.VMEM((GROUP, 2, 2, 128), F32),
            pltpu.VMEM((2, 2, 128), F32),
            pltpu.VMEM((PEERS, 2, 128), F32),
            pltpu.VMEM((2, 128), F32),
            pltpu.VMEM((2 * PEERS, 2, 128), F32),
            pltpu.VMEM((GROUP, 2, 128), F32),
            pltpu.VMEM((4, 2, 2, 128), F32),
            pltpu.VMEM((16, 2, 5, 4, 128), BF16),
            pltpu.VMEM((PEERS, 5, 4, 128), BF16),
            pltpu.VMEM((16, 2, 5, 4, 128), BF16),
            pltpu.VMEM((PEERS, 5, 4, 128), BF16),
        ]
        + [dma, dma, dma, dma((GROUP,)), dma, dma, dma((GROUP,))]
        + [dma] * 12,
        compiler_params=pltpu.CompilerParams(
            collective_id=0, has_side_effects=True, vmem_limit_bytes=48 << 20
        ),
    )(
        counts,
        *(
            pltpu.with_memory_space_constraint(array, pltpu.HBM)
            for array in (
                ids.reshape(2, 128),
                hash_scale.reshape(1, CODES),
                hash_shift.reshape(1, CODES),
                norm_gain.reshape(8, 128),
                norm_bias.reshape(8, 128),
                w_code,
                w_out,
                cotangent,
                out_bias.reshape(1, 128),
            )
        ),
    )
    emb, gcode, gout, ggain, gbias = pl.pallas_call(
        store_kernel,
        out_shape=shapes,
        in_specs=[vmem] * 5,
        out_specs=(hbm,) * 5,
        scratch_shapes=[dma((5,))],
        compiler_params=pltpu.CompilerParams(vmem_limit_bytes=4 << 20),
    )(*results)
    return emb, gcode, gout, ggain.reshape(1024), gbias.reshape(1024)


def solution(mesh):
    finer = Mesh(mesh.devices.reshape(8, 4, 4, 2), AXES)
    return jax.shard_map(
        per_device,
        mesh=finer,
        in_specs=(P(AXES), P(AXES), P(), P(), P(), P(), P(), P(), P(), P(AXES, None)),
        out_specs=(P(AXES, None), P(AXES, None), P(AXES, None), P(), P()),
        check_vma=False,
    )
```
